32 devices in a mesh: lat: 4 (over x, core), lon: 8 (over z, y).
Axes of the slice: x: 2, y: 2, z: 4, core: 2. Of those that a mesh axis runs over, the one named last changes fastest.
Arguments:
- background: bfloat16 [16, 256, 2560], P('lat', 'lon'), may hold values from -6 to 6
- band_cols: int32 [16], P('lat'), may hold values from 20 to 256, as said below
- obs_col: int32 [16, 512], P('lat', 'lon'), may hold values from 0 to 255, as said below
- obs_lev: int32 [16, 512], P('lat', 'lon'), may hold values from 0 to 39
- obs_mask: int32 [16, 512], P('lat', 'lon'), may hold values from 0 to 1, as said below
- innov: float32 [16, 512], P('lat', 'lon'), may hold values from -9 to 9
- obs_var: float32 [16, 512], P('lat', 'lon'), may hold values from 0.25 to 2.5
Outputs:
- analysis: bfloat16 [16, 256, 2560], P('lat', 'lon')
The draws below stay inside these ranges and needn't reach their ends.
Inputs may be any that keep to these rules, and one draw needn't show every extreme that they name: Band 0 has 20 columns, band 16 // 2 has 160 columns and the last band 256; columns from band_cols on are padding. `obs_col`: slot i of a band lies in the columns from i // 64 * 32 to that plus 32 - 1. An observation in use lies below its band's band_cols. No column holds more than 4 observations in use, and some column of every band holds exactly 4. `obs_mask`: 1 marks an observation in use.
All inputs are finite; a program needn't handle non-finite values.
Results may differ from the reference program's by a relative error of at most 0.0061.
Values may be sent and summed in bfloat16 or wider, within the bound.
A program may use at most 128 MiB of HBM per device.

```python
import math
import jax
import jax.numpy as jnp
from jax import lax

K = 64
LEV = 40
OC = 4
RADIUS = 8
ITERS = 4
MINCOLS = 20
C_DEV = 32
NOB_DEV = 64
W = 256
BANDS = 16
NOBS = 512
N_LON = 8


def band_counts(key):
    band_index = jnp.arange(BANDS, dtype=jnp.int32)
    jitter = jax.random.randint(jax.random.fold_in(key, 11), (BANDS,), 0, 9)
    baseline = MINCOLS + (W - MINCOLS) * band_index // (BANDS - 1)
    interior = (band_index > 0) & (band_index < BANDS - 1)
    counts = jnp.minimum(baseline + jnp.where(interior, jitter, 0), W)
    counts = jnp.where(band_index == BANDS // 2, W // 2 + C_DEV, counts)
    return counts.astype(jnp.int32)


def obs_layout(key):
    lengths = band_counts(key)
    capacity = C_DEV * OC
    block_total = BANDS * N_LON
    block_keys = jax.random.split(jax.random.fold_in(key, 23), block_total)

    def permute(sub_key):
        return jax.random.permutation(sub_key, capacity)
    orders = jax.vmap(permute)(block_keys)
    position = jnp.argsort(orders, axis=1)
    block_index = jnp.arange(block_total, dtype=jnp.int32)
    band_of = block_index // N_LON
    lane_of = block_index % N_LON
    upper = jnp.minimum(lengths, C_DEV)
    pinned_col = jax.random.randint(jax.random.fold_in(key, 31), (BANDS,), 0, upper)
    cell_col = jnp.arange(capacity, dtype=jnp.int32) // OC
    forced = (lane_of[:, None] == 0) & (cell_col[None, :] == pinned_col[band_of][:, None])
    priority = jnp.where(forced, -1, position)
    chosen = jnp.argsort(priority, axis=1, stable=True)[:, :NOB_DEV]
    column = lane_of[:, None] * C_DEV + chosen // OC
    draw_bits = jax.random.randint(jax.random.fold_in(key, 41), (block_total, NOB_DEV), 0, 8)
    kept = jnp.take_along_axis(forced, chosen, axis=1) | (column < lengths[band_of][:, None]) & (draw_bits > 0)
    return (column.reshape(BANDS, N_LON * NOB_DEV).astype(jnp.int32), kept.reshape(BANDS, N_LON * NOB_DEV).astype(jnp.int32))


def draw_band_cols(key, part):
    return band_counts(key)


def draw_obs_col(key, part):
    return obs_layout(key)[0]


def draw_obs_mask(key, part):
    return obs_layout(key)[1]


def touch_ends(array, stream_key, least, largest):
    longest = array.shape.index(max(array.shape))
    spots = []
    for shift in (0, 1):
        where = [jax.random.randint(jax.random.fold_in(stream_key, axis), (), 0, length) for axis, length in enumerate(array.shape)]
        where[longest] = (where[longest] + shift) % array.shape[longest]
        spots.append(tuple(where))
    return array.at[spots[0]].set(least).at[spots[1]].set(largest)


def block_levels(rng, extent, pieces, low, high):
    def one(dim, parts):
        steps = jax.random.uniform(jax.random.fold_in(jax.random.fold_in(rng, 6), dim), (parts,), jnp.float32, low / len(pieces), high / len(pieces))
        return jnp.repeat(jnp.exp(steps), extent[dim] // parts).reshape((-1,) + (1,) * (len(extent) - dim - 1))

    factor_of = one(*pieces[0])
    for cut in pieces[1:]:
        factor_of = factor_of * one(*cut)
    return factor_of


def centred(key, shape, scale, reach, cuts=(), held_as=jnp.bfloat16):
    gain = block_levels(key, shape, cuts, -0.22, 0.18) if cuts else 1.0
    values = jax.random.normal(key, shape, jnp.float32) * scale * gain
    return jnp.minimum(jnp.maximum(values, -reach), reach).astype(held_as)


def setup_inputs(seed: int = 0) -> dict:
    arg_keys = jax.random.split(jax.random.key(seed), 8)
    background = centred(arg_keys[0], (BANDS, W, LEV * K), 1.0, 6.0, ((0, 4), (1, 8)))
    band_cols = draw_band_cols(jax.random.fold_in(arg_keys[7], 71), 0)
    obs_col = draw_obs_col(jax.random.fold_in(arg_keys[7], 71), 0)
    obs_lev = touch_ends(jax.random.randint(arg_keys[3], (BANDS, NOBS), 0, LEV), jax.random.fold_in(arg_keys[3], 1), 0, LEV - 1).astype(jnp.int32)
    obs_mask = draw_obs_mask(jax.random.fold_in(arg_keys[7], 71), 0)
    innov = centred(arg_keys[5], (BANDS, NOBS), 1.5, 9.0, ((0, 4), (1, 8)), jnp.float32)
    obs_var = jnp.clip(jnp.exp(math.log(2.5) - 2.3025851 * jax.random.uniform(arg_keys[6], (BANDS, NOBS), jnp.float32) ** block_levels(arg_keys[6], (BANDS, NOBS), ((0, 4), (1, 8)), -0.2, 0.2)), 0.25, 2.5)
    return {"background": background, "band_cols": band_cols, "obs_col": obs_col, "obs_lev": obs_lev, "obs_mask": obs_mask, "innov": innov, "obs_var": obs_var}


EXACT_ARITHMETIC = lax.Precision.HIGHEST

def taper_weights(radius):
    half_width = radius / 2.0
    tapering = []
    for offset in range(1 - radius, radius):
        distance = abs(offset) / half_width
        if distance <= 1.0:
            weight = ((-0.25 * distance + 0.5) * distance + 0.625) * distance ** 3 - 5.0 / 3.0 * distance ** 2 + 1.0
        else:
            weight = (((distance / 12.0 - 0.5) * distance + 0.625) * distance + 5.0 / 3.0) * distance ** 2 - 5.0 * distance + 4.0 - 2.0 / (3.0 * distance)
        tapering.append(weight)
    return tapering

def centred_system(localized_weights, inflation):
    members = localized_weights.shape[-1]
    identity = jnp.eye(members, dtype=jnp.float32)
    row_mean = lax.optimization_barrier(jnp.mean(localized_weights, axis=-1))
    column_average = lax.optimization_barrier(jnp.mean(localized_weights, axis=-2))
    all_mean = lax.optimization_barrier(jnp.mean(row_mean, axis=-1))
    mean_shift = all_mean[..., None] - row_mean
    system = localized_weights - row_mean[..., :, None] - column_average[..., None, :] + all_mean[..., None, None] + (members - 1) / inflation * identity
    return (system, mean_shift)

def transform_of(system, mean_shift):
    members = system.shape[-1]
    identity = jnp.eye(members, dtype=jnp.float32)
    magnitude = jnp.sqrt(lax.optimization_barrier(jnp.sum(system * system, axis=(-2, -1))))
    root_est = system / magnitude[..., None, None]
    inv_root = jnp.broadcast_to(identity, system.shape)
    for iteration in range(ITERS):
        update = 1.5 * identity - 0.5 * jnp.einsum('...ij,...jk->...ik', inv_root, root_est, precision=EXACT_ARITHMETIC)
        if iteration + 1 < ITERS:
            root_est = jnp.einsum('...ij,...jk->...ik', root_est, update, precision=EXACT_ARITHMETIC)
        inv_root = jnp.einsum('...ij,...jk->...ik', update, inv_root, precision=EXACT_ARITHMETIC)
    half_step = jnp.einsum('...ij,...j->...i', inv_root, mean_shift, precision=EXACT_ARITHMETIC)
    mean_weight = jnp.einsum('...ij,...j->...i', inv_root, half_step, precision=EXACT_ARITHMETIC) / magnitude[..., None]
    scaling = jnp.sqrt(members - 1.0) / jnp.sqrt(magnitude)
    return inv_root * scaling[..., None, None] + mean_weight[..., :, None]

def reference(background, band_cols, obs_col, obs_lev, obs_mask, innov, obs_var):
    flattened = background.reshape(BANDS, W * LEV, K)
    row_index = (obs_col * LEV + obs_lev).astype(jnp.int32)
    picked = jnp.take_along_axis(flattened, row_index[:, :, None], axis=1).astype(jnp.float32)
    anomaly = picked - lax.optimization_barrier(jnp.mean(picked, axis=2, keepdims=True))
    mask_weight = obs_mask.astype(jnp.float32)
    obs_scale = jnp.sqrt(mask_weight / obs_var)
    depart = (obs_scale[:, :, None] * (anomaly - innov[:, :, None])).astype(jnp.bfloat16)
    depart_wide = depart.astype(jnp.float32)
    centre = lax.optimization_barrier(jnp.mean(depart_wide, axis=2, keepdims=True))
    spread = depart_wide - centre
    numerator = jnp.sum(centre * centre) + 1e-06
    denominator = jnp.sum(mask_weight) + jnp.sum(spread * spread) / (K - 1)
    inflation = numerator / denominator
    tapering = taper_weights(RADIUS)
    halo_width = RADIUS - 1
    positions = jnp.arange(W, dtype=jnp.int32)

    def one_band(band_item):
        ensemble, departures, columns_of, band_count = band_item
        outer_prod = departures[:, :, None] * departures[:, None, :]
        gram_table = jax.ops.segment_sum(outer_prod, columns_of, num_segments=W)
        localized_weights = jnp.zeros((W, K, K), jnp.float32)
        for tap_index in range(2 * halo_width + 1):
            wrapped_columns = jnp.mod(positions + (tap_index - halo_width), band_count).astype(jnp.int32)
            localized_weights = localized_weights + tapering[tap_index] * gram_table[wrapped_columns]
        system, mean_shift = centred_system(localized_weights, inflation)
        ensemble_transform = transform_of(system, mean_shift)
        field_values = ensemble.reshape(W, LEV, K).astype(jnp.float32)
        centred_ensemble_field = lax.optimization_barrier(jnp.mean(field_values, axis=2, keepdims=True))
        analysis_members = centred_ensemble_field + jnp.einsum('oqz,ozy->oqy', field_values - centred_ensemble_field, ensemble_transform, precision=EXACT_ARITHMETIC)
        analysis_members = jnp.where((positions < band_count)[:, None, None], analysis_members, 0.0)
        return analysis_members.reshape(W, LEV * K).astype(jnp.bfloat16)
    return lax.map(one_band, (background, depart_wide, obs_col, band_cols))
```

```python
import functools

import jax
import jax.numpy as jnp
from jax import lax
from jax.experimental import pallas as pl
from jax.experimental.pallas import tpu as pltpu
from jax.sharding import PartitionSpec as P

K = 64
RADIUS = 8
GROUP = 4
OC = 4
END_SLOTS = 32
FAR = 1 << 20
LANES = 128
PAIR = 2
SPAN = GROUP * K
F32 = jnp.float32
BF16 = jnp.bfloat16
MESH = pl.DeviceIdType.MESH


def taper_weights(radius):
    half_width = radius / 2.0
    tapering = []
    for offset in range(radius):
        distance = offset / half_width
        if distance <= 1.0:
            weight = (
                ((-0.25 * distance + 0.5) * distance + 0.625) * distance**3
                - 5.0 / 3.0 * distance**2
                + 1.0
            )
        else:
            weight = (
                (((distance / 12.0 - 0.5) * distance + 0.625) * distance + 5.0 / 3.0) * distance**2
                - 5.0 * distance
                + 4.0
                - 2.0 / (3.0 * distance)
            )
        tapering.append(weight)
    return tapering


def dot(left, right):
    return jnp.dot(left, right, preferred_element_type=F32)


def iota(shape, dim):
    return lax.broadcasted_iota(jnp.int32, shape, dim)


def exchange_kernel(
    lats,
    lons,
    x_hbm,
    col_hbm,
    lev_hbm,
    mask_hbm,
    innov_hbm,
    var_hbm,
    cols_hbm,
    own_ref,
    side_ref,
    info_ref,
    w_ref,
    xl_ref,
    x_v,
    col_ref,
    lev_ref,
    mask_ref,
    innov_ref,
    var_ref,
    cols_ref,
    xs,
    ends_buf,
    near_buf,
    tail_buf,
    stat_buf,
    x_sem,
    in_sem,
    near_send,
    near_recv,
    head_send,
    head_recv,
    tail_send,
    tail_recv,
    stat_send,
    stat_recv,
):
    lat, lon = lax.axis_index("lat"), lax.axis_index("lon")
    bands, columns, width = x_v.shape
    obs = col_ref.shape[1]
    devices = lats * lons
    me = lat * lons + lon
    smalls = (
        (col_hbm, col_ref),
        (lev_hbm, lev_ref),
        (mask_hbm, mask_ref),
        (innov_hbm, innov_ref),
        (var_hbm, var_ref),
        (cols_hbm, cols_ref),
    )
    loads = [
        pltpu.make_async_copy(source, target, in_sem.at[i])
        for i, (source, target) in enumerate(smalls)
    ]
    x_loads = [pltpu.make_async_copy(x_hbm.at[b], x_v.at[b], x_sem.at[b]) for b in range(bands)]
    for load in loads + x_loads:
        load.start()
    barrier = pltpu.get_barrier_semaphore()
    near_buf[...] = jnp.zeros_like(near_buf)
    tail_buf[...] = jnp.zeros_like(tail_buf)

    def peer(step):
        other = lax.rem(me + step, devices)
        return lax.div(other, lons), lax.rem(other, lons)

    def greet(step, carry):
        pl.semaphore_signal(barrier, inc=1, device_id=peer(step), device_id_type=MESH)
        return carry

    lax.fori_loop(1, devices, greet, 0)

    pairs = width // LANES
    reach = RADIUS - 1
    ends = END_SLOTS
    first = lon * columns
    for load in loads:
        load.wait()
    local_int = col_ref[...] - first
    local = local_int.astype(F32)
    mask = mask_ref[...].astype(F32)
    scale = jnp.sqrt(mask / var_ref[...])
    params = jnp.concatenate([local, lev_ref[...].astype(F32), scale, innov_ref[...]], axis=0)
    params = jnp.concatenate([params, jnp.zeros((LANES - 4 * bands, obs), F32)], axis=0)
    params = jnp.concatenate([params, jnp.zeros((LANES, LANES - obs), F32)], axis=1)
    upright = jnp.transpose(params)[:obs]
    col_ids = iota((obs, columns), 1)
    earlier = iota((obs, obs), 0) < iota((obs, obs), 1)
    slot_ids = iota((ends, obs), 0)

    def stacked(kind):
        return jnp.concatenate(
            [upright[:, kind * bands + b : kind * bands + b + 1] for b in range(bands)], axis=0
        )

    marks = []
    for b in range(bands):
        col = upright[:, b : b + 1]
        depart_scale = upright[:, 2 * bands + b : 2 * bands + b + 1]
        row = local_int[b : b + 1]
        used = mask[b : b + 1] > 0.0
        same = (col == local[b : b + 1]) & (depart_scale > 0.0) & earlier
        rank = jnp.sum(jnp.where(same, 1.0, 0.0), axis=0, keepdims=True).astype(jnp.int32)
        bases = (row, row - (columns - reach), row + first - (cols_ref[b] - reach))
        mark = []
        for base in bases:
            fits = used & (base >= 0) & (base < reach)
            slot = jnp.where(fits, base * OC + rank, -1)
            mark.append(jnp.where(slot_ids == slot, 1.0, 0.0))
        marks.append(jnp.concatenate(mark, axis=0).astype(BF16))

    levels = stacked(1).astype(jnp.int32)
    scales = stacked(2)
    gathered = []
    for b in range(bands):
        onehot = jnp.where(col_ids == upright[:, b : b + 1].astype(jnp.int32), 1.0, 0.0).astype(BF16)
        pair = lax.shift_right_logical(levels[b * obs : (b + 1) * obs], 1)
        found = jnp.zeros((obs, LANES), F32)
        x_loads[b].wait()
        for p in range(0, pairs, 2):
            got = dot(onehot, x_v[b, :, p * LANES : (p + 2) * LANES])
            found = jnp.where(pair == p, got[:, :LANES], found)
            found = jnp.where(pair == p + 1, got[:, LANES:], found)
        gathered.append(found)
    found = jnp.concatenate(gathered, axis=0)
    total = bands * obs
    low_t = iota((total, LANES), 1) < K
    even = (levels & 1) == 0
    picked = jnp.where(low_t == even, found, pltpu.roll(found, K, 1))
    anomaly = picked - jnp.mean(picked, axis=1, keepdims=True)
    departs = (scales * (anomaly - stacked(3))).astype(BF16)
    own_ref[...] = departs
    wide = departs.astype(F32)
    centre = jnp.mean(wide, axis=1, keepdims=True)
    spread = wide - centre
    numerator = jnp.sum(centre * centre, axis=0, keepdims=True)
    spread_row = jnp.sum(spread * spread, axis=0, keepdims=True)
    mask_row = jnp.sum(mask, axis=0, keepdims=True)
    denominator = jnp.sum(spread_row, axis=1, keepdims=True) * (0.5 / (K - 1)) + jnp.sum(
        mask_row, axis=1, keepdims=True
    )
    stat_buf[me] = jnp.where(iota((1, LANES), 1) == 0, numerator, denominator)

    pl.semaphore_wait(barrier, devices - 1)

    def stat_copy(slot, step, other):
        return pltpu.make_async_remote_copy(
            src_ref=stat_buf.at[slot],
            dst_ref=stat_buf.at[slot],
            send_sem=stat_send.at[step],
            recv_sem=stat_recv.at[slot],
            device_id=other,
            device_id_type=MESH,
        )

    def near_copy(kind, slot, other):
        return pltpu.make_async_remote_copy(
            src_ref=ends_buf.at[kind],
            dst_ref=near_buf.at[slot],
            send_sem=near_send.at[slot],
            recv_sem=near_recv.at[slot],
            device_id=(lat, other),
            device_id_type=MESH,
        )

    def head_copy(other):
        return pltpu.make_async_remote_copy(
            src_ref=ends_buf.at[0],
            dst_ref=near_buf.at[2],
            send_sem=head_send.at[other],
            recv_sem=head_recv,
            device_id=(lat, other),
            device_id_type=MESH,
        )

    def tail_copy(slot):
        return pltpu.make_async_remote_copy(
            src_ref=ends_buf.at[2],
            dst_ref=tail_buf.at[slot],
            send_sem=tail_send,
            recv_sem=tail_recv.at[slot],
            device_id=(lat, 0),
            device_id_type=MESH,
        )

    def send_stat(step, carry):
        stat_copy(me, step, peer(step)).start()
        return carry

    lax.fori_loop(1, devices, send_stat, 0)

    low = iota((obs, LANES), 1) < K
    for q in range(bands // PAIR):
        mark = jnp.concatenate([marks[2 * q], marks[2 * q + 1]], axis=1)
        one = departs[(2 * q) * obs : (2 * q + 1) * obs]
        two = departs[(2 * q + 1) * obs : (2 * q + 2) * obs]
        both = jnp.concatenate(
            [jnp.where(low, one.astype(F32), 0.0), jnp.where(low, 0.0, two.astype(F32))], axis=0
        ).astype(BF16)
        compact = dot(mark, both).astype(BF16)
        for kind in range(3):
            ends_buf[kind, q] = compact[kind * ends : (kind + 1) * ends]

    @pl.when(lon > 0)
    def _():
        tail_copy(lon).start()
        near_copy(0, 1, lon - 1).start()

    @pl.when(lon == 0)
    def _():
        def send(other, carry):
            head_copy(other).start()
            return carry

        lax.fori_loop(1, lons, send, 0)

    @pl.when(lon < lons - 1)
    def _():
        near_copy(1, 0, lon + 1).start()

    tapering = taper_weights(RADIUS)
    slots = obs + 3 * ends
    lane = iota((1, LANES), 1)
    lane_band, lane_col = lane // columns, lane % columns
    count = jnp.zeros((1, LANES), jnp.int32)
    for b in range(bands):
        count = jnp.where(lane_band == b, cols_ref[b], count)
    chooser = jnp.where(iota((LANES, LANES), 0) == lane_band, 1.0, 0.0).astype(BF16)
    source = dot(upright.astype(BF16), chooser).astype(jnp.int32)
    source = jnp.concatenate([source, jnp.zeros((3 * ends, LANES), jnp.int32)], axis=0)
    place = iota((slots, LANES), 0)
    nth = (place - obs) // OC
    each = ends // OC
    source = jnp.where(
        place < obs,
        source,
        jnp.where(
            place < obs + ends,
            nth - reach,
            jnp.where(place < obs + 2 * ends, nth - each + columns, nth - 2 * each + count - first),
        ),
    )
    limit = jnp.where(place < obs, count, FAR)
    away = source - lane_col
    away = jnp.where(2 * away > limit, away - count, away)
    away = jnp.where(2 * away < -limit, away + count, away)
    away = jnp.abs(away)
    weight = jnp.zeros((slots, LANES), F32)
    for t in range(RADIUS):
        weight = jnp.where(away == t, tapering[t], weight)
    w_ref[...] = weight

    rows_x = xs.shape[0] // columns
    groups = columns // GROUP
    low_x = iota((rows_x, LANES), 1) < K
    xs[...] = jnp.zeros_like(xs)

    def spread_band(b, carry):
        for p in range(pairs):
            strip = x_v[b, :, p * LANES : (p + 1) * LANES].astype(F32)
            xs[pl.ds(p, columns, stride=rows_x), :] = strip
        for g in range(groups):
            halves = []
            for c in (g * GROUP, g * GROUP + 2):
                here = xs[c * rows_x : (c + 1) * rows_x, :]
                there = xs[(c + 1) * rows_x : (c + 2) * rows_x, :]
                halves.append(
                    jnp.concatenate(
                        [
                            jnp.where(low_x, here, pltpu.roll(there, K, 1)),
                            jnp.where(low_x, pltpu.roll(here, K, 1), there),
                        ],
                        axis=0,
                    ).astype(BF16)
                )
            xl_ref[b * groups + g] = jnp.concatenate(halves, axis=1)
        return carry

    lax.fori_loop(0, bands, spread_band, 0)

    @pl.when(lon > 0)
    def _():
        near_copy(1, 0, lon - 1).wait_recv()
        head_copy(lon).wait_recv()
        tail_copy(lon).wait_send()
        near_copy(0, 1, lon - 1).wait_send()

    @pl.when(lon == 0)
    def _():
        def take(other, carry):
            head_copy(other).wait_send()
            tail_copy(other).wait_recv()
            return carry

        lax.fori_loop(1, lons, take, 0)

    @pl.when(lon < lons - 1)
    def _():
        near_copy(0, 1, lon + 1).wait_recv()
        near_copy(1, 0, lon + 1).wait_send()

    side_ref[0] = (
        near_buf[0].astype(F32) + jnp.sum(tail_buf[...].astype(F32), axis=0)
    ).astype(BF16)
    side_ref[1] = near_buf[1]
    side_ref[2] = near_buf[2]

    def take_stat(step, carry):
        stat_copy(me, step, peer(step)).wait_send()
        source = lax.rem(me + devices - step, devices)
        stat_copy(source, step, peer(step)).wait_recv()
        return carry

    lax.fori_loop(1, devices, take_stat, 0)
    stats = jnp.sum(stat_buf[...], axis=0)
    inflation = (stats[:, 0:1] + 1e-06) / stats[:, 1:2]
    shift = jnp.broadcast_to((K - 1) / inflation, (8, LANES))
    line = iota((8, LANES), 0)
    info = shift
    for b in range(bands):
        info = jnp.where(line == 1 + b, (cols_ref[b] - first).astype(F32), info)
    info_ref[...] = info


def analysis_kernel(
    own_ref,
    side_ref,
    info_ref,
    w_ref,
    xl_ref,
    out_hbm,
    dc,
    lhs,
    cf,
    cb,
    sf,
    sb,
    nf,
    nb,
    xf,
    xb,
    tf,
    uf,
    px,
    ys,
    obuf,
    out_sem,
):
    bands, columns, width = obuf.shape
    obs = own_ref.shape[0] // bands
    ends = side_ref.shape[2]
    slots = obs + 3 * ends
    pairs = width // LANES
    groups = columns // GROUP
    rows_x = ys.shape[1] // columns
    tall = 2 * rows_x
    spare = pairs
    shift = info_ref[0:1, 0:1]
    low_b = jnp.where(iota((K, LANES), 1) < K, 1.0, 0.0).astype(BF16)
    high_b = jnp.where(iota((K, LANES), 1) < K, 0.0, 1.0).astype(BF16)
    zero_b = jnp.zeros((K, LANES), BF16)
    low_x = iota((rows_x, LANES), 1) < K
    eye = jnp.where(iota((K, SPAN), 0) == iota((K, SPAN), 1) % K, 1.0, 0.0)
    batch = [(j, g) for j in range(PAIR) for g in range(groups)]
    many = len(batch)

    def block_diag(mat):
        left, right = mat[:, :LANES], mat[:, LANES:]
        return jnp.concatenate(
            [
                jnp.concatenate([left * low_b, zero_b], axis=1),
                jnp.concatenate([left * high_b, zero_b], axis=1),
                jnp.concatenate([zero_b, right * low_b], axis=1),
                jnp.concatenate([zero_b, right * high_b], axis=1),
            ],
            axis=0,
        )

    ones_bd = block_diag(jnp.ones((K, SPAN), BF16))

    def one_pair(p, carry):
        sides = jnp.concatenate([side_ref[kind, p] for kind in range(3)], axis=0).astype(F32)
        swapped = pltpu.roll(sides, K, 1)
        low_s = iota((3 * ends, LANES), 1) < K
        low_h = iota((LANES, LANES), 1) < K
        for j in range(PAIR):
            start = pl.multiple_of((p * PAIR + j) * obs, obs)
            here = jnp.where(low_s, sides, swapped) if j == 0 else jnp.where(low_s, swapped, sides)
            slot = jnp.concatenate([own_ref[pl.ds(start, obs), :].astype(F32), here], axis=0)
            dc[j] = slot - jnp.mean(slot, axis=1, keepdims=True)
            rest = jnp.concatenate(
                [slot[LANES:], jnp.zeros((2 * LANES - slots, LANES), F32)], axis=0
            )
            turned = jnp.transpose(jnp.where(low_h, slot[:LANES], rest))
            turned = jnp.concatenate([turned[:K], turned[K:]], axis=1)
            centre = jnp.mean(turned, axis=0, keepdims=True)
            lhs[j] = jnp.concatenate(
                [turned - centre, -centre, jnp.zeros((15, SPAN), F32)], axis=0
            ).astype(BF16)

        squares = []
        lane_high = jnp.where(iota((slots, LANES), 1) < K, 0, 1)
        for i, (j, g) in enumerate(batch):
            right = []
            base = (p * PAIR + j) * columns + g * GROUP
            for half in range(2):
                index = lane_high + (base + 2 * half)
                spreadw = jnp.take_along_axis(w_ref[...], index, axis=1)
                right.append((dc[j] * spreadw).astype(BF16))
            gram = dot(lhs[j, :, :slots], jnp.concatenate(right, axis=1))
            c = gram[:K]
            cf[i] = c
            cb[i] = c.astype(BF16)
            mean = gram[K : K + 1]
            line = iota((16, SPAN), 0) + 16
            tile = xl_ref[(p * PAIR + j) * groups + g, 16:32, :].astype(F32)
            px[i] = jnp.where(line == spare, mean, tile).astype(BF16)
            system = c + shift * eye
            squares.append(jnp.sum(system * system, axis=0, keepdims=True))
        squares = jnp.concatenate(squares, axis=0)
        coarse = squares.astype(BF16)
        fine = (squares - coarse.astype(F32)).astype(BF16)
        sums = dot(jnp.concatenate([coarse, fine], axis=0), ones_bd)
        frob = jnp.sqrt(sums[:many] + sums[many:])
        inv = 1.0 / frob
        scaling = jnp.sqrt((K - 1.0) * inv)
        beta = 1.0 - shift * inv
        beta1 = beta * beta * (0.75 + 0.25 * beta)
        beta2 = beta1 * beta1 * (0.75 + 0.25 * beta1)
        k1 = -inv * (1.5 * beta + 0.75 * beta * beta)
        k2 = inv * inv * (0.75 + 0.75 * beta)
        k3 = -0.25 * inv * inv * inv
        a0 = 1.0 + 0.5 * beta
        d0 = -0.5 * inv
        a1 = 1.0 + 0.5 * beta1
        e1 = 1.5 * beta1 + 0.75 * beta1 * beta1
        e2 = 0.75 + 0.75 * beta1
        c0 = (1.0 + 0.5 * beta2) * (1.0 + (0.375 + 0.125 * beta2) * beta2 * beta2)
        c1 = 0.5 + beta2 * (0.75 + beta2 * (0.9375 + 0.25 * beta2))
        c2 = 0.375 + beta2 * (0.9375 + 0.375 * beta2)
        c3 = 0.3125 + 0.25 * beta2
        rest = (1.0 - scaling * a0 * a1 * c0) * (1.0 / K)

        def members(i, j, g):
            tile = (p * PAIR + j) * groups + g
            return jnp.concatenate(
                [xl_ref[tile, :16, :], px[i], xl_ref[tile, 32:, :]], axis=0
            )

        for i, (j, g) in enumerate(batch):
            both = dot(jnp.concatenate([cb[i], members(i, j, g)], axis=0), block_diag(cb[i]))
            square = both[:K]
            sf[i] = square
            sb[i] = square.astype(BF16)
            x1 = a0[i : i + 1] * members(i, j, g).astype(F32) + d0[i : i + 1] * both[K:]
            xf[i] = x1
            xb[i] = x1.astype(BF16)
        for i in range(many):
            cube = dot(cb[i], block_diag(sb[i]))
            dev = k1[i : i + 1] * cf[i] + k2[i : i + 1] * sf[i] + k3[i : i + 1] * cube
            nf[i] = dev
            nb[i] = dev.astype(BF16)
        for i in range(many):
            both = dot(jnp.concatenate([nb[i], xb[i]], axis=0), block_diag(nb[i]))
            square = both[:K]
            sf[i] = square
            sb[i] = square.astype(BF16)
            x2 = a1[i : i + 1] * xf[i] + 0.5 * both[K:]
            xf[i] = x2
            xb[i] = x2.astype(BF16)
        for i in range(many):
            cube = dot(nb[i], block_diag(sb[i]))
            dev = e1[i : i + 1] * nf[i] + e2[i : i + 1] * sf[i] + 0.25 * cube
            cb[i] = dev.astype(BF16)
        for i in range(many):
            both = dot(jnp.concatenate([cb[i], xb[i]], axis=0), block_diag(cb[i]))
            sb[i] = both[:K].astype(BF16)
            x2 = xf[i]
            tf[i] = c2[i : i + 1] * x2 + c3[i : i + 1] * both[K:]
            uf[i] = c0[i : i + 1] * x2 + c1[i : i + 1] * both[K:]
        for i in range(many):
            quad = dot(xb[i], block_diag(sb[i]))
            xb[i] = (tf[i] + 0.0625 * quad).astype(BF16)
        for i, (j, g) in enumerate(batch):
            x4 = uf[i] + dot(xb[i], block_diag(sb[i]))
            uf[i] = x4
            step = x4[spare : spare + 1] * inv[i : i + 1]
            xb[i] = (x4 * step + members(i, j, g).astype(F32) * rest[i : i + 1]).astype(BF16)
        for i, (j, g) in enumerate(batch):
            result = scaling[i : i + 1] * uf[i] + dot(xb[i], ones_bd)
            for side in range(2):
                c = g * GROUP + 2 * side
                got = result[:, side * LANES : (side + 1) * LANES]
                even, odd = got[:rows_x], got[rows_x:]
                ys[j, c * rows_x : (c + 1) * rows_x, :] = jnp.where(low_x, even, pltpu.roll(odd, K, 1))
                ys[j, (c + 1) * rows_x : (c + 2) * rows_x, :] = jnp.where(
                    low_x, pltpu.roll(even, K, 1), odd
                )
        for j in range(PAIR):
            b = p * PAIR + j
            keep = iota((columns, LANES), 0).astype(F32) < info_ref[pl.ds(1 + b, 1), :]
            for t in range(pairs):
                obuf[b, :, t * LANES : (t + 1) * LANES] = jnp.where(
                    keep, ys[j, pl.ds(t, columns, stride=rows_x), :], 0.0
                ).astype(BF16)
            pltpu.make_async_copy(obuf.at[b], out_hbm.at[b], out_sem.at[b]).start()
        return carry

    lax.fori_loop(0, bands // PAIR, one_pair, 0)
    for b in range(bands):
        pltpu.make_async_copy(obuf.at[b], out_hbm.at[b], out_sem.at[b]).wait()


def per_device(lats, lons, background, band_cols, obs_col, obs_lev, obs_mask, innov, obs_var):
    bands, columns, width = background.shape
    obs = obs_col.shape[1]
    pairs = width // LANES
    devices = lats * lons
    vmem = pl.BlockSpec(memory_space=pltpu.VMEM)
    hbm = pl.BlockSpec(memory_space=pltpu.HBM)
    dma = pltpu.SemaphoreType.DMA
    rows_x = -(-(pairs + 1) // 8) * 8
    halves = bands // PAIR
    slots = obs + 3 * END_SLOTS
    groups = columns // GROUP
    many = PAIR * groups
    room = 16 * 1024 * 1024
    own, side, info, weight, spread = pl.pallas_call(
        functools.partial(exchange_kernel, lats, lons),
        out_shape=(
            jax.ShapeDtypeStruct((bands * obs, LANES), BF16),
            jax.ShapeDtypeStruct((3, halves, END_SLOTS, LANES), BF16),
            jax.ShapeDtypeStruct((8, LANES), F32),
            jax.ShapeDtypeStruct((slots, LANES), F32),
            jax.ShapeDtypeStruct((bands * groups, 2 * rows_x, SPAN), BF16),
        ),
        in_specs=[hbm] * 7,
        out_specs=(vmem,) * 5,
        scratch_shapes=[
            pltpu.VMEM((bands, columns, width), BF16),
            pltpu.VMEM((bands, obs), jnp.int32),
            pltpu.VMEM((bands, obs), jnp.int32),
            pltpu.VMEM((bands, obs), jnp.int32),
            pltpu.VMEM((bands, obs), F32),
            pltpu.VMEM((bands, obs), F32),
            pltpu.SMEM((bands,), jnp.int32),
            pltpu.VMEM((columns * rows_x, LANES), F32),
            pltpu.VMEM((3, halves, END_SLOTS, LANES), BF16),
            pltpu.VMEM((3, halves, END_SLOTS, LANES), BF16),
            pltpu.VMEM((lons, halves, END_SLOTS, LANES), BF16),
            pltpu.VMEM((devices, 1, LANES), F32),
            dma((bands,)),
            dma((6,)),
            dma((2,)),
            dma((2,)),
            dma((lons,)),
            dma,
            dma,
            dma((lons,)),
            dma((devices,)),
            dma((devices,)),
        ],
        compiler_params=pltpu.CompilerParams(
            collective_id=0, has_side_effects=True, vmem_limit_bytes=room
        ),
        name="exchange",
    )(*(pltpu.with_memory_space_constraint(a, pltpu.HBM) for a in (background, obs_col, obs_lev, obs_mask, innov, obs_var, band_cols)))
    return pl.pallas_call(
        analysis_kernel,
        out_shape=jax.ShapeDtypeStruct(background.shape, BF16),
        in_specs=[vmem] * 5,
        out_specs=hbm,
        scratch_shapes=[
            pltpu.VMEM((PAIR, slots, LANES), F32),
            pltpu.VMEM((PAIR, K + 16, SPAN), BF16),
            pltpu.VMEM((many, K, SPAN), F32),
            pltpu.VMEM((many, K, SPAN), BF16),
            pltpu.VMEM((many, K, SPAN), F32),
            pltpu.VMEM((many, K, SPAN), BF16),
            pltpu.VMEM((many, K, SPAN), F32),
            pltpu.VMEM((many, K, SPAN), BF16),
            pltpu.VMEM((many, 2 * rows_x, SPAN), F32),
            pltpu.VMEM((many, 2 * rows_x, SPAN), BF16),
            pltpu.VMEM((many, 2 * rows_x, SPAN), F32),
            pltpu.VMEM((many, 2 * rows_x, SPAN), F32),
            pltpu.VMEM((many, 16, SPAN), BF16),
            pltpu.VMEM((PAIR, columns * rows_x, LANES), F32),
            pltpu.VMEM((bands, columns, width), BF16),
            dma((bands,)),
        ],
        compiler_params=pltpu.CompilerParams(vmem_limit_bytes=room),
        name="analysis",
    )(own, side, info, weight, spread)


def solution(mesh):
    placed = (P("lat", "lon", None), P("lat")) + (P("lat", "lon"),) * 5
    return jax.shard_map(
        functools.partial(per_device, mesh.shape["lat"], mesh.shape["lon"]),
        mesh=mesh,
        in_specs=placed,
        out_specs=P("lat", "lon", None),
        check_vma=False,
    )
```

```python
import functools

import jax
import jax.numpy as jnp
from jax import lax
from jax.experimental import pallas as pl
from jax.experimental.pallas import tpu as pltpu
from jax.sharding import PartitionSpec as P

K = 64
RADIUS = 8
GROUP = 4
OC = 4
END_SLOTS = 32
FAR = 1 << 20
LANES = 128
PAIR = 2
SPAN = GROUP * K
F32 = jnp.float32
BF16 = jnp.bfloat16
MESH = pl.DeviceIdType.MESH


def taper_weights(radius):
    half_width = radius / 2.0
    tapering = []
    for offset in range(radius):
        distance = offset / half_width
        if distance <= 1.0:
            weight = (
                ((-0.25 * distance + 0.5) * distance + 0.625) * distance**3
                - 5.0 / 3.0 * distance**2
                + 1.0
            )
        else:
            weight = (
                (((distance / 12.0 - 0.5) * distance + 0.625) * distance + 5.0 / 3.0) * distance**2
                - 5.0 * distance
                + 4.0
                - 2.0 / (3.0 * distance)
            )
        tapering.append(weight)
    return tapering


def dot(left, right):
    return jnp.dot(left, right, preferred_element_type=F32)


def iota(shape, dim):
    return lax.broadcasted_iota(jnp.int32, shape, dim)


def block_diag(mat):
    lanes = iota((K, LANES), 1)
    low = jnp.where(lanes < K, 1.0, 0.0).astype(BF16)
    high = jnp.where(lanes < K, 0.0, 1.0).astype(BF16)
    zero = jnp.zeros((K, LANES), BF16)
    left, right = mat[:, :LANES], mat[:, LANES:]
    return jnp.concatenate(
        [
            jnp.concatenate([left * low, zero], axis=1),
            jnp.concatenate([left * high, zero], axis=1),
            jnp.concatenate([zero, right * low], axis=1),
            jnp.concatenate([zero, right * high], axis=1),
        ],
        axis=0,
    )


def exchange_kernel(
    lats,
    lons,
    x_hbm,
    col_hbm,
    lev_hbm,
    mask_hbm,
    innov_hbm,
    var_hbm,
    cols_hbm,
    c_out,
    s_out,
    q_out,
    p_out,
    x_out,
    norm_out,
    info_out,
    x_v,
    col_ref,
    lev_ref,
    mask_ref,
    innov_ref,
    var_ref,
    cols_ref,
    xs,
    own,
    weights,
    ends_buf,
    near_buf,
    tail_buf,
    stat_buf,
    x_sem,
    in_sem,
    near_send,
    near_recv,
    head_send,
    head_recv,
    tail_send,
    tail_recv,
    stat_send,
    stat_recv,
):
    lat, lon = lax.axis_index("lat"), lax.axis_index("lon")
    bands, columns, width = x_v.shape
    obs = col_ref.shape[1]
    devices = lats * lons
    me = lat * lons + lon
    smalls = (
        (col_hbm, col_ref),
        (lev_hbm, lev_ref),
        (mask_hbm, mask_ref),
        (innov_hbm, innov_ref),
        (var_hbm, var_ref),
        (cols_hbm, cols_ref),
    )
    loads = [
        pltpu.make_async_copy(source, target, in_sem.at[i])
        for i, (source, target) in enumerate(smalls)
    ]
    x_loads = [pltpu.make_async_copy(x_hbm.at[b], x_v.at[b], x_sem.at[b]) for b in range(bands)]
    for load in loads + x_loads:
        load.start()
    barrier = pltpu.get_barrier_semaphore()
    near_buf[...] = jnp.zeros_like(near_buf)
    tail_buf[...] = jnp.zeros_like(tail_buf)

    for other in range(devices):

        @pl.when(me != other)
        def _():
            pl.semaphore_signal(
                barrier, inc=1, device_id=(other // lons, other % lons), device_id_type=MESH
            )

    pairs = width // LANES
    reach = RADIUS - 1
    ends = END_SLOTS
    first = lon * columns
    for load in loads:
        load.wait()
    mask = mask_ref[...].astype(F32)
    used_all = mask > 0.0
    local_int = jnp.where(used_all, col_ref[...] - first, -columns)
    local = local_int.astype(F32)
    lev = lev_ref[...]
    spot = (lax.shift_right_logical(lev, 1) * columns + col_ref[...] - first) * 2 + (lev & 1)
    scale = jnp.sqrt(mask / var_ref[...])
    params = jnp.concatenate([local, spot.astype(F32), scale, innov_ref[...]], axis=0)
    params = jnp.concatenate([params, jnp.zeros((LANES - 4 * bands, obs), F32)], axis=0)
    params = jnp.concatenate([params, jnp.zeros((LANES, LANES - obs), F32)], axis=1)
    upright = jnp.transpose(params)[:obs]
    earlier = iota((obs, obs), 0) < iota((obs, obs), 1)
    slot_ids = iota((ends, obs), 0)

    def stacked(kind):
        return jnp.concatenate(
            [upright[:, kind * bands + b : kind * bands + b + 1] for b in range(bands)], axis=0
        )

    marks = []
    for b in range(bands):
        row = local_int[b : b + 1]
        used = used_all[b : b + 1]
        same = (upright[:, b : b + 1] == local[b : b + 1]) & earlier
        rank = jnp.sum(jnp.where(same, 1.0, 0.0), axis=0, keepdims=True).astype(jnp.int32)
        bases = (row, row - (columns - reach), row + first - (cols_ref[b] - reach))
        mark = []
        for base in bases:
            fits = used & (base >= 0) & (base < reach)
            slot = jnp.where(fits, base * OC + rank, -1)
            mark.append(jnp.where(slot_ids == slot, 1.0, 0.0))
        marks.append(jnp.concatenate(mark, axis=0).astype(BF16))

    spots = stacked(1).astype(jnp.int32)
    scales = stacked(2)
    depth = pairs * columns
    gathered = []
    for b in range(bands):
        index = lax.shift_right_logical(spots[b * obs : (b + 1) * obs], 1)
        onehot = jnp.where(iota((obs, depth), 1) == index, 1.0, 0.0).astype(BF16)
        x_loads[b].wait()
        field = jnp.concatenate(
            [x_v[b, :, p * LANES : (p + 1) * LANES] for p in range(pairs)], axis=0
        )
        gathered.append(dot(onehot, field))
    found = jnp.concatenate(gathered, axis=0)
    total = bands * obs
    low_t = iota((total, LANES), 1) < K
    even = (spots & 1) == 0
    picked = jnp.where(low_t == even, found, pltpu.roll(found, K, 1))
    anomaly = picked - jnp.mean(picked, axis=1, keepdims=True)
    departs = (scales * (anomaly - stacked(3))).astype(BF16)
    wide = departs.astype(F32)
    own[...] = wide
    centre = jnp.mean(wide, axis=1, keepdims=True)
    spread = wide - centre
    numerator = jnp.sum(centre * centre, axis=0, keepdims=True)
    spread_row = jnp.sum(spread * spread, axis=0, keepdims=True)
    mask_row = jnp.sum(mask, axis=0, keepdims=True)
    denominator = jnp.sum(spread_row, axis=1, keepdims=True) * (0.5 / (K - 1)) + jnp.sum(
        mask_row, axis=1, keepdims=True
    )
    stat_buf[me] = jnp.where(iota((1, LANES), 1) == 0, numerator, denominator)

    pl.semaphore_wait(barrier, devices - 1)

    def stat_copy(slot, size, other):
        return pltpu.make_async_remote_copy(
            src_ref=stat_buf.at[pl.ds(slot, size)],
            dst_ref=stat_buf.at[pl.ds(slot, size)],
            send_sem=stat_send,
            recv_sem=stat_recv,
            device_id=(other // lons, other % lons),
            device_id_type=MESH,
        )

    def near_copy(kind, slot, other):
        return pltpu.make_async_remote_copy(
            src_ref=ends_buf.at[kind],
            dst_ref=near_buf.at[slot],
            send_sem=near_send.at[slot],
            recv_sem=near_recv.at[slot],
            device_id=(lat, other),
            device_id_type=MESH,
        )

    def head_copy(other):
        return pltpu.make_async_remote_copy(
            src_ref=ends_buf.at[0],
            dst_ref=near_buf.at[2],
            send_sem=head_send.at[other],
            recv_sem=head_recv,
            device_id=(lat, other),
            device_id_type=MESH,
        )

    def tail_copy(slot):
        return pltpu.make_async_remote_copy(
            src_ref=ends_buf.at[2],
            dst_ref=tail_buf.at[slot],
            send_sem=tail_send,
            recv_sem=tail_recv,
            device_id=(lat, 0),
            device_id_type=MESH,
        )

    for other in range(devices):

        @pl.when(me != other)
        def _():
            stat_copy(me, 1, other).start()

    low = iota((obs, LANES), 1) < K
    for q in range(bands // PAIR):
        mark = jnp.concatenate([marks[2 * q], marks[2 * q + 1]], axis=1)
        one = wide[(2 * q) * obs : (2 * q + 1) * obs]
        two = wide[(2 * q + 1) * obs : (2 * q + 2) * obs]
        both = jnp.concatenate(
            [jnp.where(low, one, 0.0), jnp.where(low, 0.0, two)], axis=0
        ).astype(BF16)
        compact = dot(mark, both).astype(BF16)
        for kind in range(3):
            ends_buf[kind, q] = compact[kind * ends : (kind + 1) * ends]

    @pl.when(lon > 0)
    def _():
        tail_copy(lon).start()
        near_copy(0, 1, lon - 1).start()

    @pl.when(lon == 0)
    def _():
        for other in range(1, lons):
            head_copy(other).start()

    @pl.when(lon < lons - 1)
    def _():
        near_copy(1, 0, lon + 1).start()

    tapering = taper_weights(RADIUS)
    slots = obs + 2 * ends
    lane = iota((1, LANES), 1)
    lane_band, lane_col = lane // columns, lane % columns
    count = jnp.zeros((1, LANES), jnp.int32)
    for b in range(bands):
        count = jnp.where(lane_band == b, cols_ref[b], count)
    chooser = jnp.where(iota((LANES, LANES), 0) == lane_band, 1.0, 0.0).astype(BF16)
    source = dot(upright.astype(BF16), chooser).astype(jnp.int32)
    nth = iota((ends, LANES), 0) // OC

    def taper(place, limit):
        away = place - lane_col
        away = jnp.where(2 * away > limit, away - limit, away)
        away = jnp.where(2 * away < -limit, away + limit, away)
        away = jnp.abs(away)
        weight = jnp.zeros(place.shape, F32)
        for t in range(RADIUS):
            weight = jnp.where(away == t, tapering[t], weight)
        return weight.astype(BF16)

    near_own = taper(source, count)
    near_left = taper(nth - reach, FAR)
    near_right = taper(nth + columns, FAR)
    near_head = taper(nth + count - first, FAR)
    weights[0] = jnp.concatenate([near_own, near_right, near_head], axis=0)
    weights[1] = jnp.concatenate([near_own, near_left, near_head], axis=0)

    rows_x = xs.shape[0] // columns
    groups = columns // GROUP
    low_x = iota((rows_x, LANES), 1) < K
    xs[...] = jnp.zeros_like(xs)

    def spread_band(b, carry):
        for p in range(pairs):
            strip = x_v[b, :, p * LANES : (p + 1) * LANES].astype(F32)
            xs[pl.ds(p, columns, stride=rows_x), :] = strip
        for g in range(groups):
            halves = []
            for c in (g * GROUP, g * GROUP + 2):
                here = xs[c * rows_x : (c + 1) * rows_x, :]
                there = xs[(c + 1) * rows_x : (c + 2) * rows_x, :]
                halves.append(
                    jnp.concatenate(
                        [
                            jnp.where(low_x, here, pltpu.roll(there, K, 1)),
                            jnp.where(low_x, pltpu.roll(here, K, 1), there),
                        ],
                        axis=0,
                    ).astype(BF16)
                )
            x_out[b * groups + g] = jnp.concatenate(halves, axis=1)
        return carry

    lax.fori_loop(0, bands, spread_band, 0)

    eye = jnp.where(iota((K, SPAN), 0) == iota((K, SPAN), 1) % K, 1.0, 0.0)
    low_e = iota((2 * ends, LANES), 1) < K
    spare = pairs
    expand_row = iota((LANES, SPAN), 0) - iota((LANES, SPAN), 1) // K
    row_id = iota((16, SPAN), 0) + 16

    def early(p, which, chosen, extra):
        swapped = pltpu.roll(extra, K, 1)
        made = []
        for j in range(PAIR):
            b = p * PAIR + j
            here = jnp.where(low_e, extra, swapped) if j == 0 else jnp.where(low_e, swapped, extra)
            mine = own[pl.ds(pl.multiple_of(b * obs, obs), obs), :]
            slot = jnp.concatenate([mine, here], axis=0)
            spread = slot - jnp.mean(slot, axis=1, keepdims=True)
            turned = jnp.transpose(slot)[:K]
            centre = jnp.mean(turned, axis=0, keepdims=True)
            left = jnp.concatenate(
                [turned - centre, -centre, jnp.zeros((15, slots), F32)], axis=0
            ).astype(BF16)
            made.append((left, spread))
        places = [(j, g) for j in range(PAIR) for g in chosen]
        at = [(p * PAIR + j) * groups + g for j, g in places]
        right = []
        for j, g in places:
            picker = jnp.where(
                expand_row == (p * PAIR + j) * columns + g * GROUP, 1.0, 0.0
            ).astype(BF16)
            wide_w = dot(weights[which], picker)
            spread = made[j][1]
            right.append(
                jnp.concatenate(
                    [
                        (spread * wide_w[:, :LANES]).astype(BF16),
                        (spread * wide_w[:, LANES:]).astype(BF16),
                    ],
                    axis=1,
                )
            )
        narrow, fields = [], []
        for (j, g), i, r in zip(places, at, right):
            gram = dot(made[j][0], r)
            c = gram[:K]
            c_out[i] = c
            narrow.append(c.astype(BF16))
            mean = gram[K : K + 1]
            old = x_out[i]
            middle = jnp.where(row_id == spare, mean, old[16:32].astype(F32)).astype(BF16)
            field = jnp.concatenate([old[:16], middle, old[32:]], axis=0)
            x_out[i] = field
            fields.append(field)
            norm_out[0, pl.ds(i, 1), :] = jnp.sum(c * c, axis=0, keepdims=True)
            norm_out[1, pl.ds(i, 1), :] = jnp.sum(c * eye, axis=0, keepdims=True)
        squares = []
        for i, n, f in zip(at, narrow, fields):
            both = dot(jnp.concatenate([n, f], axis=0), block_diag(n))
            s_out[i] = both[:K]
            p_out[i] = both[K:]
            squares.append(both[:K].astype(BF16))
        for i, n, q in zip(at, narrow, squares):
            q_out[i] = dot(n, block_diag(q))

    @pl.when(lon > 0)
    def _():
        head_copy(lon).wait_recv()

    @pl.when(lon < lons - 1)
    def _():
        near_copy(0, 1, lon + 1).wait_recv()

    edge = -(-reach // GROUP)

    def inner(p, carry):
        extra = jnp.concatenate([near_buf[1, p], near_buf[2, p]], axis=0).astype(F32)
        early(p, 0, range(edge, groups), extra)
        return carry

    lax.fori_loop(0, bands // PAIR, inner, 0)

    @pl.when(lon > 0)
    def _():
        near_copy(1, 0, lon - 1).wait_recv()

    @pl.when(lon == 0)
    def _():
        pltpu.make_async_remote_copy(
            src_ref=tail_buf.at[pl.ds(1, lons - 1)],
            dst_ref=tail_buf.at[pl.ds(1, lons - 1)],
            send_sem=tail_send,
            recv_sem=tail_recv,
            device_id=(lat, 0),
            device_id_type=MESH,
        ).wait_recv()

    def outer(p, carry):
        ahead = near_buf[0, p].astype(F32)
        for other in range(1, lons):
            ahead = ahead + tail_buf[other, p].astype(F32)
        extra = jnp.concatenate([ahead, near_buf[2, p].astype(F32)], axis=0)
        early(p, 1, range(edge), extra)
        return carry

    lax.fori_loop(0, bands // PAIR, outer, 0)

    @pl.when(lon > 0)
    def _():
        tail_copy(lon).wait_send()
        near_copy(0, 1, lon - 1).wait_send()

    @pl.when(lon == 0)
    def _():
        for other in range(1, lons):
            head_copy(other).wait_send()

    @pl.when(lon < lons - 1)
    def _():
        near_copy(1, 0, lon + 1).wait_send()

    everyone = stat_copy(0, devices - 1, 0)
    everyone.wait_send()
    everyone.wait_recv()
    stats = jnp.sum(stat_buf[...], axis=0)
    inflation = (stats[:, 0:1] + 1e-06) / stats[:, 1:2]
    shift = jnp.broadcast_to((K - 1) / inflation, (8, LANES))
    line = iota((8, LANES), 0)
    info = shift
    for b in range(bands):
        info = jnp.where(line == 1 + b, (cols_ref[b] - first).astype(F32), info)
    info_out[...] = info


def analysis_kernel(
    c_ref,
    s_ref,
    q_ref,
    p_ref,
    x_ref,
    norm_ref,
    info_ref,
    out_hbm,
    coef,
    ys,
    obuf,
    out_sem,
):
    bands, columns, width = obuf.shape
    pairs = width // LANES
    groups = columns // GROUP
    rows_x = ys.shape[1] // columns
    spare = pairs
    shift = info_ref[0:1, 0:1]
    low_x = iota((rows_x, LANES), 1) < K
    batch = [(j, g) for j in range(PAIR) for g in range(groups)]
    many = len(batch)
    ones_bd = block_diag(jnp.ones((K, SPAN), BF16))

    squares = norm_ref[0] + shift * (2.0 * norm_ref[1] + shift)
    coarse = squares.astype(BF16)
    fine = (squares - coarse.astype(F32)).astype(BF16)
    sums = dot(jnp.concatenate([coarse, fine], axis=0), ones_bd)
    size = squares.shape[0]
    inv = lax.rsqrt(sums[:size] + sums[size:])
    scaling = jnp.sqrt((K - 1.0) * inv)
    beta = 1.0 - shift * inv
    beta1 = beta * beta * (0.75 + 0.25 * beta)
    beta2 = beta1 * beta1 * (0.75 + 0.25 * beta1)
    a0 = 1.0 + 0.5 * beta
    a1 = 1.0 + 0.5 * beta1
    half1 = 0.5 / a1
    c0 = (1.0 + 0.5 * beta2) * (1.0 + (0.375 + 0.125 * beta2) * beta2 * beta2)
    c1 = 0.5 + beta2 * (0.75 + beta2 * (0.9375 + 0.25 * beta2))
    c2 = 0.375 + beta2 * (0.9375 + 0.375 * beta2)
    c3 = 0.3125 + 0.25 * beta2
    up, down = c1 / c0, c0 / c1
    whole = a0 * a1 * c0
    table = (
        -inv * (1.5 * beta + 0.75 * beta * beta) * half1,
        inv * inv * (0.75 + 0.75 * beta) * half1,
        -0.25 * inv * inv * inv * half1,
        -0.5 * inv / a0,
        2.0 * a1 * up * (1.5 * beta1 + 0.75 * beta1 * beta1),
        4.0 * a1 * a1 * up * (0.75 + 0.75 * beta1),
        2.0 * a1 * a1 * a1 * up,
        c2 / c0 * down * down,
        c3 / c0 * down * down * down,
        0.0625 / c0 * (down * down) * (down * down),
        whole * whole * inv,
        (1.0 - scaling * whole) * (1.0 / K),
        scaling * whole,
    )
    for t, value in enumerate(table):
        coef[t] = value

    def one_pair(p, carry):
        at = [(p * PAIR + j) * groups + g for j, g in batch]

        def k(t, i):
            return coef[t, pl.ds(i, 1), :]

        def wide_x(i):
            return x_ref[i].astype(F32)

        dev, dev_b, mem, mem_b = [], [], [], []
        for i in at:
            m = k(0, i) * c_ref[i] + k(1, i) * s_ref[i] + k(2, i) * q_ref[i]
            x = wide_x(i) + k(3, i) * p_ref[i]
            dev.append(m)
            dev_b.append(m.astype(BF16))
            mem.append(x)
            mem_b.append(x.astype(BF16))
        both = [
            dot(jnp.concatenate([n, x], axis=0), block_diag(n)) for n, x in zip(dev_b, mem_b)
        ]
        square = [v[:K] for v in both]
        mem = [x + v[K:] for x, v in zip(mem, both)]
        cube = [dot(n, block_diag(s.astype(BF16))) for n, s in zip(dev_b, square)]
        dev_b = [
            (k(4, i) * n + k(5, i) * s + k(6, i) * q).astype(BF16)
            for i, n, s, q in zip(at, dev, square, cube)
        ]
        mem_b = [x.astype(BF16) for x in mem]
        both = [
            dot(jnp.concatenate([n, x], axis=0), block_diag(n)) for n, x in zip(dev_b, mem_b)
        ]
        fixed = [v[:K].astype(BF16) for v in both]
        part = [
            k(7, i) * x + k(8, i) * v[K:] for i, x, v in zip(at, mem, both)
        ]
        mem = [x + v[K:] for x, v in zip(mem, both)]
        quad = [dot(x, block_diag(f)) for x, f in zip(mem_b, fixed)]
        part = [
            (y + k(9, i) * v).astype(BF16) for i, y, v in zip(at, part, quad)
        ]
        mem = [x + dot(y, block_diag(f)) for x, y, f in zip(mem, part, fixed)]
        mean_b = [
            (x * (x[spare : spare + 1] * k(10, i)) + wide_x(i) * k(11, i)).astype(BF16)
            for i, x in zip(at, mem)
        ]
        for i, (j, g), x, m in zip(at, batch, mem, mean_b):
            result = k(12, i) * x + dot(m, ones_bd)
            for side in range(2):
                c = g * GROUP + 2 * side
                got = result[:, side * LANES : (side + 1) * LANES]
                even, odd = got[:rows_x], got[rows_x:]
                ys[j, c * rows_x : (c + 1) * rows_x, :] = jnp.where(low_x, even, pltpu.roll(odd, K, 1))
                ys[j, (c + 1) * rows_x : (c + 2) * rows_x, :] = jnp.where(
                    low_x, pltpu.roll(even, K, 1), odd
                )
        for j in range(PAIR):
            b = p * PAIR + j
            keep = iota((columns, LANES), 0).astype(F32) < info_ref[pl.ds(1 + b, 1), :]
            for t in range(pairs):
                obuf[b, :, t * LANES : (t + 1) * LANES] = jnp.where(
                    keep, ys[j, pl.ds(t, columns, stride=rows_x), :], 0.0
                ).astype(BF16)
            pltpu.make_async_copy(obuf.at[b], out_hbm.at[b], out_sem.at[b]).start()
        return carry

    lax.fori_loop(0, bands // PAIR, one_pair, 0)
    for b in range(bands):
        pltpu.make_async_copy(obuf.at[b], out_hbm.at[b], out_sem.at[b]).wait()


def per_device(lats, lons, background, band_cols, obs_col, obs_lev, obs_mask, innov, obs_var):
    bands, columns, width = background.shape
    obs = obs_col.shape[1]
    pairs = width // LANES
    devices = lats * lons
    vmem = pl.BlockSpec(memory_space=pltpu.VMEM)
    hbm = pl.BlockSpec(memory_space=pltpu.HBM)
    dma = pltpu.SemaphoreType.DMA
    rows_x = -(-(pairs + 1) // 8) * 8
    halves = bands // PAIR
    slots = obs + 2 * END_SLOTS
    total = bands * columns // GROUP
    room = 16 * 1024 * 1024
    arrays = (background, obs_col, obs_lev, obs_mask, innov, obs_var, band_cols)
    made = pl.pallas_call(
        functools.partial(exchange_kernel, lats, lons),
        out_shape=(
            jax.ShapeDtypeStruct((total, K, SPAN), F32),
            jax.ShapeDtypeStruct((total, K, SPAN), F32),
            jax.ShapeDtypeStruct((total, K, SPAN), F32),
            jax.ShapeDtypeStruct((total, 2 * rows_x, SPAN), F32),
            jax.ShapeDtypeStruct((total, 2 * rows_x, SPAN), BF16),
            jax.ShapeDtypeStruct((2, total, SPAN), F32),
            jax.ShapeDtypeStruct((8, LANES), F32),
        ),
        in_specs=[hbm] * 7,
        out_specs=(vmem,) * 7,
        scratch_shapes=[
            pltpu.VMEM((bands, columns, width), BF16),
            pltpu.VMEM((bands, obs), jnp.int32),
            pltpu.VMEM((bands, obs), jnp.int32),
            pltpu.VMEM((bands, obs), jnp.int32),
            pltpu.VMEM((bands, obs), F32),
            pltpu.VMEM((bands, obs), F32),
            pltpu.SMEM((bands,), jnp.int32),
            pltpu.VMEM((columns * rows_x, LANES), F32),
            pltpu.VMEM((bands * obs, LANES), F32),
            pltpu.VMEM((2, slots, LANES), BF16),
            pltpu.VMEM((3, halves, END_SLOTS, LANES), BF16),
            pltpu.VMEM((3, halves, END_SLOTS, LANES), BF16),
            pltpu.VMEM((lons, halves, END_SLOTS, LANES), BF16),
            pltpu.VMEM((devices, 1, LANES), F32),
            dma((bands,)),
            dma((6,)),
            dma((2,)),
            dma((2,)),
            dma((lons,)),
            dma,
            dma,
            dma,
            dma,
            dma,
        ],
        compiler_params=pltpu.CompilerParams(
            collective_id=0, has_side_effects=True, vmem_limit_bytes=room
        ),
        name="exchange",
    )(*(pltpu.with_memory_space_constraint(a, pltpu.HBM) for a in arrays))
    return pl.pallas_call(
        analysis_kernel,
        out_shape=jax.ShapeDtypeStruct(background.shape, BF16),
        in_specs=[vmem] * 7,
        out_specs=hbm,
        scratch_shapes=[
            pltpu.VMEM((13, total, SPAN), F32),
            pltpu.VMEM((PAIR, columns * rows_x, LANES), F32),
            pltpu.VMEM((bands, columns, width), BF16),
            dma((bands,)),
        ],
        compiler_params=pltpu.CompilerParams(vmem_limit_bytes=room),
        name="analysis",
    )(*made)


def solution(mesh):
    placed = (P("lat", "lon", None), P("lat")) + (P("lat", "lon"),) * 5
    return jax.shard_map(
        functools.partial(per_device, mesh.shape["lat"], mesh.shape["lon"]),
        mesh=mesh,
        in_specs=placed,
        out_specs=P("lat", "lon", None),
        check_vma=False,
    )
```

```python
import functools

import jax
import jax.numpy as jnp
from jax import lax
from jax.experimental import pallas as pl
from jax.experimental.pallas import tpu as pltpu
from jax.sharding import PartitionSpec as P

K = 64
RADIUS = 8
GROUP = 4
OC = 4
END_SLOTS = 32
FAR = 1 << 20
GAP_OWN = 16
GAP_EARLY = 12
GAP_LATE = 8
SHARED = 4
LANES = 128
PAIR = 2
SPAN = GROUP * K
F32 = jnp.float32
BF16 = jnp.bfloat16
MESH = pl.DeviceIdType.MESH


def taper_weights(radius):
    half_width = radius / 2.0
    tapering = []
    for offset in range(radius):
        distance = offset / half_width
        if distance <= 1.0:
            weight = (
                ((-0.25 * distance + 0.5) * distance + 0.625) * distance**3
                - 5.0 / 3.0 * distance**2
                + 1.0
            )
        else:
            weight = (
                (((distance / 12.0 - 0.5) * distance + 0.625) * distance + 5.0 / 3.0) * distance**2
                - 5.0 * distance
                + 4.0
                - 2.0 / (3.0 * distance)
            )
        tapering.append(weight)
    return tapering


def dot(left, right):
    return jnp.dot(left, right, preferred_element_type=F32)


def iota(shape, dim):
    return lax.broadcasted_iota(jnp.int32, shape, dim)


def block_diag(mat):
    lanes = iota((K, LANES), 1)
    zero = jnp.zeros((K, LANES), BF16)
    left, right = mat[:, :LANES], mat[:, LANES:]
    return jnp.concatenate(
        [
            jnp.concatenate([jnp.where(lanes < K, left, zero), zero], axis=1),
            jnp.concatenate([jnp.where(lanes < K, zero, left), zero], axis=1),
            jnp.concatenate([zero, jnp.where(lanes < K, right, zero)], axis=1),
            jnp.concatenate([zero, jnp.where(lanes < K, zero, right)], axis=1),
        ],
        axis=0,
    )


def wavefront(tasks, gap):
    started = []
    step = 0
    while step < len(tasks) or started:
        if step < len(tasks):
            started.append((step, tasks[step]))
        left = []
        for begin, task in started:
            if (step - begin) % gap == 0:
                try:
                    next(task)
                except StopIteration:
                    continue
            left.append((begin, task))
        started = left
        step += 1


def exchange_kernel(
    lats,
    lons,
    x_hbm,
    col_hbm,
    lev_hbm,
    mask_hbm,
    innov_hbm,
    var_hbm,
    cols_hbm,
    r_out,
    info_out,
    c_out,
    s_out,
    q_out,
    p_out,
    x_out,
    norm,
    coef,
    x_v,
    col_ref,
    lev_ref,
    mask_ref,
    innov_ref,
    var_ref,
    cols_ref,
    xs,
    own,
    weights,
    w_side,
    c_own,
    ends_buf,
    near_buf,
    tail_buf,
    stat_buf,
    x_sem,
    in_sem,
    near_send,
    near_recv,
    head_send,
    head_recv,
    tail_send,
    tail_recv,
    stat_send,
    stat_recv,
):
    lat, lon = lax.axis_index("lat"), lax.axis_index("lon")
    bands, columns, width = x_v.shape
    obs = col_ref.shape[1]
    devices = lats * lons
    me = lat * lons + lon
    smalls = (
        (col_hbm, col_ref),
        (lev_hbm, lev_ref),
        (mask_hbm, mask_ref),
        (innov_hbm, innov_ref),
        (var_hbm, var_ref),
        (cols_hbm, cols_ref),
    )
    loads = [
        pltpu.make_async_copy(source, target, in_sem.at[i])
        for i, (source, target) in enumerate(smalls)
    ]
    x_loads = [pltpu.make_async_copy(x_hbm.at[b], x_v.at[b], x_sem.at[b]) for b in range(bands)]
    for load in loads + x_loads:
        load.start()
    barrier = pltpu.get_barrier_semaphore()
    near_buf[...] = jnp.zeros_like(near_buf)
    tail_buf[...] = jnp.zeros_like(tail_buf)

    for other in range(devices):

        @pl.when(me != other)
        def _():
            pl.semaphore_signal(
                barrier, inc=1, device_id=(other // lons, other % lons), device_id_type=MESH
            )

    xs[...] = jnp.zeros_like(xs)
    norm[...] = jnp.zeros_like(norm)
    pairs = width // LANES
    reach = RADIUS - 1
    ends = END_SLOTS
    first = lon * columns
    for load in loads:
        load.wait()
    mask = mask_ref[...].astype(F32)
    used_all = mask > 0.0
    local_int = jnp.where(used_all, col_ref[...] - first, -columns)
    local = local_int.astype(F32)
    lev = lev_ref[...]
    spot = (lax.shift_right_logical(lev, 1) * columns + col_ref[...] - first) * 2 + (lev & 1)
    scale = jnp.sqrt(mask / var_ref[...])
    params = jnp.concatenate([local, spot.astype(F32), scale, innov_ref[...]], axis=0)
    params = jnp.concatenate([params, jnp.zeros((LANES - 4 * bands, obs), F32)], axis=0)
    params = jnp.concatenate([params, jnp.zeros((LANES, LANES - obs), F32)], axis=1)
    upright = jnp.transpose(params)[:obs]
    earlier = iota((obs, obs), 0) < iota((obs, obs), 1)
    slot_ids = iota((ends, obs), 0)

    def stacked(kind):
        return jnp.concatenate(
            [upright[:, kind * bands + b : kind * bands + b + 1] for b in range(bands)], axis=0
        )

    marks = []
    for b in range(bands):
        row = local_int[b : b + 1]
        used = used_all[b : b + 1]
        same = (upright[:, b : b + 1] == local[b : b + 1]) & earlier
        rank = jnp.sum(jnp.where(same, 1.0, 0.0), axis=0, keepdims=True).astype(jnp.int32)
        bases = (row, row - (columns - reach), row + first - (cols_ref[b] - reach))
        mark = []
        for base in bases:
            fits = used & (base >= 0) & (base < reach)
            slot = jnp.where(fits, base * OC + rank, -1)
            mark.append(jnp.where(slot_ids == slot, 1.0, 0.0))
        marks.append(jnp.concatenate(mark, axis=0).astype(BF16))

    tapering = taper_weights(RADIUS)
    lane = iota((1, LANES), 1)
    lane_band, lane_col = lane // columns, lane % columns
    count = jnp.zeros((1, LANES), jnp.int32)
    for b in range(bands):
        count = jnp.where(lane_band == b, cols_ref[b], count)
    chooser = jnp.where(iota((LANES, LANES), 0) == lane_band, 1.0, 0.0).astype(BF16)
    source = dot(upright.astype(BF16), chooser).astype(jnp.int32)
    nth = iota((ends, LANES), 0) // OC

    def taper(place, limit):
        away = place - lane_col
        away = jnp.where(2 * away > limit, away - limit, away)
        away = jnp.where(2 * away < -limit, away + limit, away)
        away = jnp.abs(away)
        weight = jnp.zeros(place.shape, F32)
        for t in range(RADIUS):
            weight = jnp.where(away == t, tapering[t], weight)
        return weight.astype(BF16)

    near_own = taper(source, count)
    near_left = taper(nth - reach, FAR)
    near_right = taper(nth + columns, FAR)
    near_head = taper(nth + count - first, FAR)
    beside = (
        jnp.concatenate([near_right, near_head], axis=0),
        jnp.concatenate([near_left, near_head], axis=0),
    )
    weights[0] = jnp.concatenate([near_own, beside[0]], axis=0)
    weights[1] = jnp.concatenate([near_own, beside[1]], axis=0)

    spots = stacked(1).astype(jnp.int32)
    scales = stacked(2)
    depth = pairs * columns
    gathered = []
    for b in range(bands):
        index = lax.shift_right_logical(spots[b * obs : (b + 1) * obs], 1)
        onehot = jnp.where(iota((obs, depth), 1) == index, 1.0, 0.0).astype(BF16)
        x_loads[b].wait()
        field = jnp.concatenate(
            [x_v[b, :, p * LANES : (p + 1) * LANES] for p in range(pairs)], axis=0
        )
        gathered.append(dot(onehot, field))
    found = jnp.concatenate(gathered, axis=0)
    total = bands * obs
    low_t = iota((total, LANES), 1) < K
    even = (spots & 1) == 0
    picked = jnp.where(low_t == even, found, pltpu.roll(found, K, 1))
    anomaly = picked - jnp.mean(picked, axis=1, keepdims=True)
    departs = (scales * (anomaly - stacked(3))).astype(BF16)
    wide = departs.astype(F32)
    own[...] = wide
    centre = jnp.mean(wide, axis=1, keepdims=True)
    spread = wide - centre
    numerator = jnp.sum(centre * centre, axis=0, keepdims=True)
    spread_row = jnp.sum(spread * spread, axis=0, keepdims=True)
    mask_row = jnp.sum(mask, axis=0, keepdims=True)
    denominator = jnp.sum(spread_row, axis=1, keepdims=True) * (0.5 / (K - 1)) + jnp.sum(
        mask_row, axis=1, keepdims=True
    )
    stat_buf[me] = jnp.where(iota((1, LANES), 1) == 0, numerator, denominator)

    low = iota((obs, LANES), 1) < K
    for q in range(bands // PAIR):
        mark = jnp.concatenate([marks[2 * q], marks[2 * q + 1]], axis=1)
        one = wide[(2 * q) * obs : (2 * q + 1) * obs]
        two = wide[(2 * q + 1) * obs : (2 * q + 2) * obs]
        both = jnp.concatenate(
            [jnp.where(low, one, 0.0), jnp.where(low, 0.0, two)], axis=0
        ).astype(BF16)
        compact = dot(mark, both).astype(BF16)
        for kind in range(3):
            ends_buf[kind, q] = compact[kind * ends : (kind + 1) * ends]

    rows_x = xs.shape[0] // columns
    groups = columns // GROUP
    low_x = iota((rows_x, LANES), 1) < K
    def spread_band(b, carry):
        for p in range(pairs):
            strip = x_v[b, :, p * LANES : (p + 1) * LANES].astype(F32)
            xs[pl.ds(p, columns, stride=rows_x), :] = strip
        for g in range(groups):
            halves = []
            for c in (g * GROUP, g * GROUP + 2):
                here = xs[c * rows_x : (c + 1) * rows_x, :]
                there = xs[(c + 1) * rows_x : (c + 2) * rows_x, :]
                halves.append(
                    jnp.concatenate(
                        [
                            jnp.where(low_x, here, pltpu.roll(there, K, 1)),
                            jnp.where(low_x, pltpu.roll(here, K, 1), there),
                        ],
                        axis=0,
                    ).astype(BF16)
                )
            x_out[b * groups + g] = jnp.concatenate(halves, axis=1)
        return carry

    eye = jnp.where(iota((K, SPAN), 0) == iota((K, SPAN), 1) % K, 1.0, 0.0)
    spare = pairs
    expand_row = iota((LANES, SPAN), 0) - iota((LANES, SPAN), 1) // K
    row_id = iota((16, SPAN), 0) + 16

    edge = -(-reach // GROUP)

    def half_gram(slot):
        spread = slot - jnp.mean(slot, axis=1, keepdims=True)
        rows = slot.shape[0]
        square = jnp.concatenate([slot, jnp.zeros((LANES - rows, LANES), F32)], axis=0)
        turned = jnp.transpose(square)[:K, :rows]
        centre = jnp.mean(turned, axis=0, keepdims=True)
        left = jnp.concatenate([turned - centre, -centre, jnp.zeros((15, rows), F32)], axis=0)
        return left.astype(BF16), spread

    def weighted(spread, wide_w):
        return jnp.concatenate(
            [
                (spread * wide_w[:, :LANES]).astype(BF16),
                (spread * wide_w[:, LANES:]).astype(BF16),
            ],
            axis=1,
        )

    def own_part(p, carry):
        made = []
        for j in range(PAIR):
            start = pl.multiple_of((p * PAIR + j) * obs, obs)
            made.append(half_gram(own[pl.ds(start, obs), :]))

        def column_group(j, g):
            i = (p * PAIR + j) * groups + g
            picker = jnp.where(
                expand_row == (p * PAIR + j) * columns + g * GROUP, 1.0, 0.0
            ).astype(BF16)
            wide_w = dot(weights[1 if g < edge else 0], picker)
            yield
            w_side[i] = wide_w[obs:]
            gram = dot(made[j][0], weighted(made[j][1], wide_w[:obs]))
            yield
            c_own[i] = gram

        wavefront([column_group(j, g) for j in range(PAIR) for g in range(groups)], GAP_OWN)
        return carry

    soon = lon < lons // 2
    bands_before = jnp.where(soon, bands, 0)
    pairs_before = jnp.where(soon, bands // PAIR, 0)
    lax.fori_loop(0, bands_before, spread_band, 0)
    lax.fori_loop(0, pairs_before, own_part, 0)

    pl.semaphore_wait(barrier, devices - 1)

    def stat_copy(slot, size, other):
        return pltpu.make_async_remote_copy(
            src_ref=stat_buf.at[pl.ds(slot, size)],
            dst_ref=stat_buf.at[pl.ds(slot, size)],
            send_sem=stat_send,
            recv_sem=stat_recv,
            device_id=(other // lons, other % lons),
            device_id_type=MESH,
        )

    def near_copy(kind, slot, other):
        return pltpu.make_async_remote_copy(
            src_ref=ends_buf.at[kind],
            dst_ref=near_buf.at[slot],
            send_sem=near_send.at[slot],
            recv_sem=near_recv.at[slot],
            device_id=(lat, other),
            device_id_type=MESH,
        )

    def head_copy(other):
        return pltpu.make_async_remote_copy(
            src_ref=ends_buf.at[0],
            dst_ref=near_buf.at[2],
            send_sem=head_send.at[other],
            recv_sem=head_recv,
            device_id=(lat, other),
            device_id_type=MESH,
        )

    def tail_copy(slot):
        return pltpu.make_async_remote_copy(
            src_ref=ends_buf.at[2],
            dst_ref=tail_buf.at[slot],
            send_sem=tail_send,
            recv_sem=tail_recv,
            device_id=(lat, 0),
            device_id_type=MESH,
        )

    @pl.when(lon < lons - 1)
    def _():
        near_copy(1, 0, lon + 1).start()

    @pl.when(lon > 0)
    def _():
        near_copy(0, 1, lon - 1).start()
        tail_copy(lon).start()

    @pl.when(lon == 0)
    def _():
        for other in range(lons - 1, 0, -1):
            head_copy(other).start()

    for other in range(devices):

        @pl.when(me != other)
        def _():
            stat_copy(me, 1, other).start()

    lax.fori_loop(bands_before, bands, spread_band, 0)
    lax.fori_loop(pairs_before, bands // PAIR, own_part, 0)

    def early(chosen, extras, block, offset):
        made = []
        low_e = iota(extras[0].shape, 1) < K
        skip = 2 * ends - extras[0].shape[0]
        for extra in extras:
            swapped = pltpu.roll(extra, K, 1)
            made.append(half_gram(jnp.where(low_e, extra, swapped)))
            made.append(half_gram(jnp.where(low_e, swapped, extra)))
        places = [(j, j * groups + g) for j in range(bands) for g in chosen]

        def column_group(line, j, i):
            gram = c_own[i] + dot(made[j][0], weighted(made[j][1], w_side[i, skip:]))
            yield
            c = gram[:K]
            c_out[i] = c
            narrow = c.astype(BF16)
            mean = gram[K : K + 1]
            old = x_out[i]
            middle = jnp.where(row_id == spare, mean, old[16:32].astype(F32)).astype(BF16)
            field = jnp.concatenate([old[:16], middle, old[32:]], axis=0)
            x_out[i] = field
            norm[block, 0, line : line + 1, :] = jnp.sum(c * c, axis=0, keepdims=True)
            norm[block, 1, line : line + 1, :] = jnp.sum(c * eye, axis=0, keepdims=True)
            both = dot(jnp.concatenate([narrow, field], axis=0), block_diag(narrow))
            yield
            s_out[i] = both[:K]
            p_out[i] = both[K:]
            cube = dot(narrow, block_diag(both[:K].astype(BF16)))
            yield
            q_out[i] = cube

        return [column_group(offset + n, j, i) for n, (j, i) in enumerate(places)]

    @pl.when(lon > 0)
    def _():
        head_copy(lon).wait_recv()

    halves = bands // PAIR
    centre_groups = range(edge, groups - edge)
    heads = [near_buf[2, p].astype(F32) for p in range(halves)]
    wavefront(early(centre_groups, heads, 0, 0), GAP_EARLY)

    everyone = stat_copy(0, devices - 1, 0)
    everyone.wait_send()
    everyone.wait_recv()
    stats = jnp.sum(stat_buf[...], axis=0)
    inflation = (stats[:, 0:1] + 1e-06) / stats[:, 1:2]
    shift = (K - 1) / inflation
    line = iota((8, LANES), 0)
    info = jnp.zeros((8, LANES), F32)
    for b in range(bands):
        info = jnp.where(line == b, (cols_ref[b] - first).astype(F32), info)
    info_out[...] = info
    ones_bd = block_diag(jnp.ones((K, SPAN), BF16))

    def settle(block):
        squares = norm[block, 0] + shift * (2.0 * norm[block, 1] + shift)
        coarse = squares.astype(BF16)
        fine = (squares - coarse.astype(F32)).astype(BF16)
        sums = dot(jnp.concatenate([coarse, fine], axis=0), ones_bd)
        size = squares.shape[0]
        inv = lax.rsqrt(sums[:size] + sums[size:])
        scaling = jnp.sqrt((K - 1.0) * inv)
        beta = 1.0 - shift * inv
        beta1 = beta * beta * (0.75 + 0.25 * beta)
        beta2 = beta1 * beta1 * (0.75 + 0.25 * beta1)
        a0 = 1.0 + 0.5 * beta
        a1 = 1.0 + 0.5 * beta1
        half1 = 0.5 / a1
        c0 = (1.0 + 0.5 * beta2) * (1.0 + (0.375 + 0.125 * beta2) * beta2 * beta2)
        c1 = 0.5 + beta2 * (0.75 + beta2 * (0.9375 + 0.25 * beta2))
        c2 = 0.375 + beta2 * (0.9375 + 0.375 * beta2)
        c3 = 0.3125 + 0.25 * beta2
        up, down = c1 / c0, c0 / c1
        whole = a0 * a1 * c0
        table = (
            -inv * (1.5 * beta + 0.75 * beta * beta) * half1,
            inv * inv * (0.75 + 0.75 * beta) * half1,
            -0.25 * inv * inv * inv * half1,
            -0.5 * inv / a0,
            2.0 * a1 * up * (1.5 * beta1 + 0.75 * beta1 * beta1),
            4.0 * a1 * a1 * up * (0.75 + 0.75 * beta1),
            2.0 * a1 * a1 * a1 * up,
            c2 / c0 * down * down,
            c3 / c0 * down * down * down,
            0.0625 / c0 * (down * down) * (down * down),
            whole * whole * inv,
            (1.0 - scaling * whole) * (1.0 / K),
            scaling * whole,
        )
        for t, value in enumerate(table):
            coef[block, t] = value

    def finish(work):
        def k(t, w):
            return coef[w[0], t, w[1] : w[1] + 1, :]

        def wide_x(w):
            return x_out[w[2]].astype(F32)

        held = {}

        def column_group(n, w):
            i = w[2]
            m = k(0, w) * c_out[i] + k(1, w) * s_out[i] + k(2, w) * q_out[i]
            x = wide_x(w) + k(3, w) * p_out[i]
            m_b = m.astype(BF16)
            both = dot(jnp.concatenate([m_b, x.astype(BF16)], axis=0), block_diag(m_b))
            yield
            square = both[:K]
            cube = dot(m_b, block_diag(square.astype(BF16)))
            x = x + both[K:]
            yield
            m_b = (k(4, w) * m + k(5, w) * square + k(6, w) * cube).astype(BF16)
            x_b = x.astype(BF16)
            both = dot(jnp.concatenate([m_b, x_b], axis=0), block_diag(m_b))
            yield
            fixed = block_diag(both[:K].astype(BF16))
            quad = dot(x_b, fixed)
            part = k(7, w) * x + k(8, w) * both[K:]
            x = x + both[K:]
            yield
            last = dot((part + k(9, w) * quad).astype(BF16), fixed)
            yield
            x = x + last
            step = x[spare : spare + 1] * k(10, w)
            held[n] = (x * step + wide_x(w) * k(11, w)).astype(BF16)
            if n % SHARED == SHARED - 1 or n + 1 == len(work):
                first_n = n - n % SHARED
                stack = jnp.concatenate([held[v] for v in range(first_n, n + 1)], axis=0)
                means = dot(stack, ones_bd)
                rows = stack.shape[0] // (n + 1 - first_n)
                for v in range(first_n, n + 1):
                    held[v] = means[(v - first_n) * rows : (v - first_n + 1) * rows]
            yield
            yield
            r_out[i] = k(12, w) * x + held[n]

        return [column_group(n, w) for n, w in enumerate(work)]

    def lines(block, offset, chosen):
        places = [b * groups + g for b in range(bands) for g in chosen]
        return [(block, offset + n, i) for n, i in enumerate(places)]

    settle(0)
    wavefront(finish(lines(0, 0, centre_groups)), GAP_LATE)

    @pl.when(lon < lons - 1)
    def _():
        near_copy(0, 1, lon + 1).wait_recv()

    @pl.when(lon > 0)
    def _():
        near_copy(1, 0, lon - 1).wait_recv()

    @pl.when(lon == 0)
    def _():
        pltpu.make_async_remote_copy(
            src_ref=tail_buf.at[pl.ds(1, lons - 1)],
            dst_ref=tail_buf.at[pl.ds(1, lons - 1)],
            send_sem=tail_send,
            recv_sem=tail_recv,
            device_id=(lat, 0),
            device_id_type=MESH,
        ).wait_recv()

    lefts, rights = [], []
    for p in range(halves):
        ahead = near_buf[0, p].astype(F32)
        for other in range(1, lons):
            ahead = ahead + tail_buf[other, p].astype(F32)
        lefts.append(jnp.concatenate([ahead, heads[p]], axis=0))
        rights.append(jnp.concatenate([near_buf[1, p].astype(F32), heads[p]], axis=0))
    left_groups, right_groups = range(edge), range(groups - edge, groups)
    wavefront(
        early(right_groups, rights, 1, 0) + early(left_groups, lefts, 1, bands * edge), GAP_EARLY
    )
    settle(1)
    wavefront(
        finish(lines(1, 0, right_groups) + lines(1, bands * edge, left_groups)), GAP_LATE
    )

    @pl.when(lon > 0)
    def _():
        tail_copy(lon).wait_send()
        near_copy(0, 1, lon - 1).wait_send()

    @pl.when(lon == 0)
    def _():
        for other in range(1, lons):
            head_copy(other).wait_send()

    @pl.when(lon < lons - 1)
    def _():
        near_copy(1, 0, lon + 1).wait_send()


def layout_kernel(r_ref, info_ref, out_hbm, ys, obuf, out_sem):
    bands, columns, width = obuf.shape
    pairs = width // LANES
    groups = columns // GROUP
    rows_x = ys.shape[1] // columns
    low_x = iota((rows_x, LANES), 1) < K

    def write(b):
        return pltpu.make_async_copy(obuf.at[b], out_hbm.at[b], out_sem.at[b])

    for b in range(bands):
        slot = b % PAIR
        for g in range(groups):
            result = r_ref[b * groups + g]
            for side in range(2):
                c = g * GROUP + 2 * side
                got = result[:, side * LANES : (side + 1) * LANES]
                even, odd = got[:rows_x], got[rows_x:]
                ys[slot, c * rows_x : (c + 1) * rows_x, :] = jnp.where(
                    low_x, even, pltpu.roll(odd, K, 1)
                )
                ys[slot, (c + 1) * rows_x : (c + 2) * rows_x, :] = jnp.where(
                    low_x, pltpu.roll(even, K, 1), odd
                )
        keep = iota((columns, LANES), 0).astype(F32) < info_ref[b : b + 1, :]
        for t in range(pairs):
            obuf[b, :, t * LANES : (t + 1) * LANES] = jnp.where(
                keep, ys[slot, pl.ds(t, columns, stride=rows_x), :], 0.0
            ).astype(BF16)
        write(b).start()
    for b in range(bands):
        write(b).wait()


def per_device(lats, lons, background, band_cols, obs_col, obs_lev, obs_mask, innov, obs_var):
    bands, columns, width = background.shape
    obs = obs_col.shape[1]
    pairs = width // LANES
    devices = lats * lons
    vmem = pl.BlockSpec(memory_space=pltpu.VMEM)
    hbm = pl.BlockSpec(memory_space=pltpu.HBM)
    dma = pltpu.SemaphoreType.DMA
    rows_x = -(-(pairs + 1) // 8) * 8
    halves = bands // PAIR
    slots = obs + 2 * END_SLOTS
    total = bands * columns // GROUP
    rim = 2 * -(-(RADIUS - 1) // GROUP) * bands
    most = -(-max(rim, total - rim) // 8) * 8
    room = 16 * 1024 * 1024
    arrays = (background, obs_col, obs_lev, obs_mask, innov, obs_var, band_cols)
    groups_f32 = pltpu.VMEM((total, K, SPAN), F32)
    result, info = pl.pallas_call(
        functools.partial(exchange_kernel, lats, lons),
        out_shape=(
            jax.ShapeDtypeStruct((total, 2 * rows_x, SPAN), F32),
            jax.ShapeDtypeStruct((8, LANES), F32),
        ),
        in_specs=[hbm] * 7,
        out_specs=(vmem,) * 2,
        scratch_shapes=[
            groups_f32,
            groups_f32,
            groups_f32,
            pltpu.VMEM((total, 2 * rows_x, SPAN), F32),
            pltpu.VMEM((total, 2 * rows_x, SPAN), BF16),
            pltpu.VMEM((2, 2, most, SPAN), F32),
            pltpu.VMEM((2, 13, most, SPAN), F32),
            pltpu.VMEM((bands, columns, width), BF16),
            pltpu.VMEM((bands, obs), jnp.int32),
            pltpu.VMEM((bands, obs), jnp.int32),
            pltpu.VMEM((bands, obs), jnp.int32),
            pltpu.VMEM((bands, obs), F32),
            pltpu.VMEM((bands, obs), F32),
            pltpu.SMEM((bands,), jnp.int32),
            pltpu.VMEM((columns * rows_x, LANES), F32),
            pltpu.VMEM((bands * obs, LANES), F32),
            pltpu.VMEM((2, slots, LANES), BF16),
            pltpu.VMEM((total, 2 * END_SLOTS, SPAN), F32),
            pltpu.VMEM((total, K + 16, SPAN), F32),
            pltpu.VMEM((3, halves, END_SLOTS, LANES), BF16),
            pltpu.VMEM((3, halves, END_SLOTS, LANES), BF16),
            pltpu.VMEM((lons, halves, END_SLOTS, LANES), BF16),
            pltpu.VMEM((devices, 1, LANES), F32),
            dma((bands,)),
            dma((6,)),
            dma((2,)),
            dma((2,)),
            dma((lons,)),
            dma,
            dma,
            dma,
            dma,
            dma,
        ],
        compiler_params=pltpu.CompilerParams(
            collective_id=0, has_side_effects=True, vmem_limit_bytes=2 * room
        ),
        name="exchange",
    )(*(pltpu.with_memory_space_constraint(a, pltpu.HBM) for a in arrays))
    return pl.pallas_call(
        layout_kernel,
        out_shape=jax.ShapeDtypeStruct(background.shape, BF16),
        in_specs=[vmem] * 2,
        out_specs=hbm,
        scratch_shapes=[
            pltpu.VMEM((PAIR, columns * rows_x, LANES), F32),
            pltpu.VMEM((bands, columns, width), BF16),
            dma((bands,)),
        ],
        compiler_params=pltpu.CompilerParams(vmem_limit_bytes=room),
        name="layout",
    )(result, info)


def solution(mesh):
    placed = (P("lat", "lon", None), P("lat")) + (P("lat", "lon"),) * 5
    return jax.shard_map(
        functools.partial(per_device, mesh.shape["lat"], mesh.shape["lon"]),
        mesh=mesh,
        in_specs=placed,
        out_specs=P("lat", "lon", None),
        check_vma=False,
    )
```

```python
import functools

import jax
import jax.numpy as jnp
from jax import lax
from jax.experimental import pallas as pl
from jax.experimental.pallas import tpu as pltpu
from jax.sharding import PartitionSpec as P

K = 64
RADIUS = 8
GROUP = 4
OC = 4
END_SLOTS = 32
FAR = 1 << 20
GAP_OWN = 16
GAP_EARLY = 12
GAP_LATE = 8
SHARED = 4
LANES = 128
PAIR = 2
SPAN = GROUP * K
F32 = jnp.float32
BF16 = jnp.bfloat16
MESH = pl.DeviceIdType.MESH


def taper_weights(radius):
    half_width = radius / 2.0
    tapering = []
    for offset in range(radius):
        distance = offset / half_width
        if distance <= 1.0:
            weight = (
                ((-0.25 * distance + 0.5) * distance + 0.625) * distance**3
                - 5.0 / 3.0 * distance**2
                + 1.0
            )
        else:
            weight = (
                (((distance / 12.0 - 0.5) * distance + 0.625) * distance + 5.0 / 3.0) * distance**2
                - 5.0 * distance
                + 4.0
                - 2.0 / (3.0 * distance)
            )
        tapering.append(weight)
    return tapering


def dot(left, right):
    return jnp.dot(left, right, preferred_element_type=F32)


def iota(shape, dim):
    return lax.broadcasted_iota(jnp.int32, shape, dim)


def block_diag(mat):
    lanes = iota((K, LANES), 1)
    zero = jnp.zeros((K, LANES), BF16)
    left, right = mat[:, :LANES], mat[:, LANES:]
    return jnp.concatenate(
        [
            jnp.concatenate([jnp.where(lanes < K, left, zero), zero], axis=1),
            jnp.concatenate([jnp.where(lanes < K, zero, left), zero], axis=1),
            jnp.concatenate([zero, jnp.where(lanes < K, right, zero)], axis=1),
            jnp.concatenate([zero, jnp.where(lanes < K, zero, right)], axis=1),
        ],
        axis=0,
    )


def wavefront(tasks, gap):
    started = []
    step = 0
    while step < len(tasks) or started:
        if step < len(tasks):
            started.append((step, tasks[step]))
        left = []
        for begin, task in started:
            if (step - begin) % gap == 0:
                try:
                    next(task)
                except StopIteration:
                    continue
            left.append((begin, task))
        started = left
        step += 1


def exchange_kernel(
    lats,
    lons,
    x_hbm,
    col_hbm,
    lev_hbm,
    mask_hbm,
    innov_hbm,
    var_hbm,
    cols_hbm,
    r_out,
    info_out,
    c_out,
    s_out,
    q_out,
    p_out,
    x_out,
    norm,
    coef,
    x_v,
    col_ref,
    lev_ref,
    mask_ref,
    innov_ref,
    var_ref,
    cols_ref,
    xs,
    own,
    weights,
    w_side,
    c_own,
    ends_buf,
    near_buf,
    tail_buf,
    stat_buf,
    x_sem,
    in_sem,
    near_send,
    near_recv,
    head_send,
    head_recv,
    tail_send,
    tail_recv,
    stat_send,
    stat_recv,
):
    lat, lon = lax.axis_index("lat"), lax.axis_index("lon")
    bands, columns, width = x_v.shape
    obs = col_ref.shape[1]
    devices = lats * lons
    me = lat * lons + lon
    smalls = (
        (col_hbm, col_ref),
        (lev_hbm, lev_ref),
        (mask_hbm, mask_ref),
        (innov_hbm, innov_ref),
        (var_hbm, var_ref),
        (cols_hbm, cols_ref),
    )
    loads = [
        pltpu.make_async_copy(source, target, in_sem.at[i])
        for i, (source, target) in enumerate(smalls)
    ]
    x_loads = [pltpu.make_async_copy(x_hbm.at[b], x_v.at[b], x_sem.at[b]) for b in range(bands)]
    for load in loads + x_loads:
        load.start()
    barrier = pltpu.get_barrier_semaphore()
    near_buf[...] = jnp.zeros_like(near_buf)
    tail_buf[...] = jnp.zeros_like(tail_buf)

    for other in range(devices):

        @pl.when(me != other)
        def _():
            pl.semaphore_signal(
                barrier, inc=1, device_id=(other // lons, other % lons), device_id_type=MESH
            )

    xs[...] = jnp.zeros_like(xs)
    norm[...] = jnp.zeros_like(norm)
    pairs = width // LANES
    reach = RADIUS - 1
    ends = END_SLOTS
    first = lon * columns
    for load in loads:
        load.wait()
    mask = mask_ref[...].astype(F32)
    used_all = mask > 0.0
    local_int = jnp.where(used_all, col_ref[...] - first, -columns)
    local = local_int.astype(F32)
    lev = lev_ref[...]
    spot = (lax.shift_right_logical(lev, 1) * columns + col_ref[...] - first) * 2 + (lev & 1)
    scale = jnp.sqrt(mask / var_ref[...])
    params = jnp.concatenate([local, spot.astype(F32), scale, innov_ref[...]], axis=0)
    params = jnp.concatenate([params, jnp.zeros((LANES - 4 * bands, obs), F32)], axis=0)
    params = jnp.concatenate([params, jnp.zeros((LANES, LANES - obs), F32)], axis=1)
    upright = jnp.transpose(params)[:obs]
    earlier = iota((obs, obs), 0) < iota((obs, obs), 1)
    slot_ids = iota((ends, obs), 0)

    def stacked(kind):
        return jnp.concatenate(
            [upright[:, kind * bands + b : kind * bands + b + 1] for b in range(bands)], axis=0
        )

    marks = []
    for b in range(bands):
        row = local_int[b : b + 1]
        used = used_all[b : b + 1]
        same = (upright[:, b : b + 1] == local[b : b + 1]) & earlier
        rank = jnp.sum(jnp.where(same, 1.0, 0.0), axis=0, keepdims=True).astype(jnp.int32)
        bases = (row, row - (columns - reach), row + first - (cols_ref[b] - reach))
        mark = []
        for base in bases:
            fits = used & (base >= 0) & (base < reach)
            slot = jnp.where(fits, base * OC + rank, -1)
            mark.append(jnp.where(slot_ids == slot, 1.0, 0.0))
        marks.append(jnp.concatenate(mark, axis=0).astype(BF16))

    tapering = taper_weights(RADIUS)
    lane = iota((1, LANES), 1)
    lane_band, lane_col = lane // columns, lane % columns
    count = jnp.zeros((1, LANES), jnp.int32)
    for b in range(bands):
        count = jnp.where(lane_band == b, cols_ref[b], count)
    chooser = jnp.where(iota((LANES, LANES), 0) == lane_band, 1.0, 0.0).astype(BF16)
    source = dot(upright.astype(BF16), chooser).astype(jnp.int32)
    nth = iota((ends, LANES), 0) // OC

    def taper(place, limit):
        away = place - lane_col
        away = jnp.where(2 * away > limit, away - limit, away)
        away = jnp.where(2 * away < -limit, away + limit, away)
        away = jnp.abs(away)
        weight = jnp.zeros(place.shape, F32)
        for t in range(RADIUS):
            weight = jnp.where(away == t, tapering[t], weight)
        return weight.astype(BF16)

    near_own = taper(source, count)
    near_left = taper(nth - reach, FAR)
    near_right = taper(nth + columns, FAR)
    near_head = taper(nth + count - first, FAR)
    beside = (
        jnp.concatenate([near_right, near_head], axis=0),
        jnp.concatenate([near_left, near_head], axis=0),
    )
    weights[0] = jnp.concatenate([near_own, beside[0]], axis=0)
    weights[1] = jnp.concatenate([near_own, beside[1]], axis=0)

    spots = stacked(1).astype(jnp.int32)
    scales = stacked(2)
    depth = pairs * columns
    gathered = []
    for b in range(bands):
        index = lax.shift_right_logical(spots[b * obs : (b + 1) * obs], 1)
        onehot = jnp.where(iota((obs, depth), 1) == index, 1.0, 0.0).astype(BF16)
        x_loads[b].wait()
        field = jnp.concatenate(
            [x_v[b, :, p * LANES : (p + 1) * LANES] for p in range(pairs)], axis=0
        )
        gathered.append(dot(onehot, field))
    found = jnp.concatenate(gathered, axis=0)
    total = bands * obs
    low_t = iota((total, LANES), 1) < K
    even = (spots & 1) == 0
    picked = jnp.where(low_t == even, found, pltpu.roll(found, K, 1))
    anomaly = picked - jnp.mean(picked, axis=1, keepdims=True)
    departs = (scales * (anomaly - stacked(3))).astype(BF16)
    wide = departs.astype(F32)
    own[...] = wide
    centre = jnp.mean(wide, axis=1, keepdims=True)
    spread = wide - centre
    numerator = jnp.sum(centre * centre, axis=0, keepdims=True)
    spread_row = jnp.sum(spread * spread, axis=0, keepdims=True)
    mask_row = jnp.sum(mask, axis=0, keepdims=True)
    denominator = jnp.sum(spread_row, axis=1, keepdims=True) * (0.5 / (K - 1)) + jnp.sum(
        mask_row, axis=1, keepdims=True
    )
    stat_buf[me] = jnp.where(iota((1, LANES), 1) == 0, numerator, denominator)

    def compact_ends():
        low = iota((obs, LANES), 1) < K
        for q in range(bands // PAIR):
            mark = jnp.concatenate([marks[2 * q], marks[2 * q + 1]], axis=1)
            one = wide[(2 * q) * obs : (2 * q + 1) * obs]
            two = wide[(2 * q + 1) * obs : (2 * q + 2) * obs]
            both = jnp.concatenate(
                [jnp.where(low, one, 0.0), jnp.where(low, 0.0, two)], axis=0
            ).astype(BF16)
            compact = dot(mark, both).astype(BF16)
            for kind in range(3):
                ends_buf[kind, q] = compact[kind * ends : (kind + 1) * ends]

    soon = lon < lons // 2
    pl.when(soon)(compact_ends)

    rows_x = xs.shape[0] // columns
    groups = columns // GROUP
    low_x = iota((rows_x, LANES), 1) < K
    def spread_band(b, carry):
        for p in range(pairs):
            strip = x_v[b, :, p * LANES : (p + 1) * LANES].astype(F32)
            xs[pl.ds(p, columns, stride=rows_x), :] = strip
        for g in range(groups):
            halves = []
            for c in (g * GROUP, g * GROUP + 2):
                here = xs[c * rows_x : (c + 1) * rows_x, :]
                there = xs[(c + 1) * rows_x : (c + 2) * rows_x, :]
                halves.append(
                    jnp.concatenate(
                        [
                            jnp.where(low_x, here, pltpu.roll(there, K, 1)),
                            jnp.where(low_x, pltpu.roll(here, K, 1), there),
                        ],
                        axis=0,
                    ).astype(BF16)
                )
            x_out[b * groups + g] = jnp.concatenate(halves, axis=1)
        return carry

    eye = jnp.where(iota((K, SPAN), 0) == iota((K, SPAN), 1) % K, 1.0, 0.0)
    spare = pairs
    expand_row = iota((LANES, SPAN), 0) - iota((LANES, SPAN), 1) // K
    row_id = iota((16, SPAN), 0) + 16

    edge = -(-reach // GROUP)

    def half_gram(slot):
        spread = slot - jnp.mean(slot, axis=1, keepdims=True)
        rows = slot.shape[0]
        square = jnp.concatenate([slot, jnp.zeros((LANES - rows, LANES), F32)], axis=0)
        turned = jnp.transpose(square)[:K, :rows]
        centre = jnp.mean(turned, axis=0, keepdims=True)
        left = jnp.concatenate([turned - centre, -centre, jnp.zeros((15, rows), F32)], axis=0)
        return left.astype(BF16), spread

    def weighted(spread, wide_w):
        return jnp.concatenate(
            [
                (spread * wide_w[:, :LANES]).astype(BF16),
                (spread * wide_w[:, LANES:]).astype(BF16),
            ],
            axis=1,
        )

    def own_part(p, carry):
        made = []
        for j in range(PAIR):
            start = pl.multiple_of((p * PAIR + j) * obs, obs)
            made.append(half_gram(own[pl.ds(start, obs), :]))

        def column_group(j, g):
            i = (p * PAIR + j) * groups + g
            picker = jnp.where(
                expand_row == (p * PAIR + j) * columns + g * GROUP, 1.0, 0.0
            ).astype(BF16)
            wide_w = dot(weights[1 if g < edge else 0], picker)
            yield
            w_side[i] = wide_w[obs:]
            gram = dot(made[j][0], weighted(made[j][1], wide_w[:obs]))
            yield
            c_own[i] = gram

        wavefront([column_group(j, g) for j in range(PAIR) for g in range(groups)], GAP_OWN)
        return carry

    bands_before = jnp.where(soon, bands, 0)
    pairs_before = jnp.where(soon, bands // PAIR, 0)
    lax.fori_loop(0, bands_before, spread_band, 0)
    lax.fori_loop(0, pairs_before, own_part, 0)

    pl.semaphore_wait(barrier, devices - 1)

    def stat_copy(slot, size, other):
        return pltpu.make_async_remote_copy(
            src_ref=stat_buf.at[pl.ds(slot, size)],
            dst_ref=stat_buf.at[pl.ds(slot, size)],
            send_sem=stat_send,
            recv_sem=stat_recv,
            device_id=(other // lons, other % lons),
            device_id_type=MESH,
        )

    def near_copy(kind, slot, other):
        return pltpu.make_async_remote_copy(
            src_ref=ends_buf.at[kind],
            dst_ref=near_buf.at[slot],
            send_sem=near_send.at[slot],
            recv_sem=near_recv.at[slot],
            device_id=(lat, other),
            device_id_type=MESH,
        )

    def head_copy(other):
        return pltpu.make_async_remote_copy(
            src_ref=ends_buf.at[0],
            dst_ref=near_buf.at[2],
            send_sem=head_send.at[other],
            recv_sem=head_recv,
            device_id=(lat, other),
            device_id_type=MESH,
        )

    def tail_copy(slot):
        return pltpu.make_async_remote_copy(
            src_ref=ends_buf.at[2],
            dst_ref=tail_buf.at[slot],
            send_sem=tail_send,
            recv_sem=tail_recv,
            device_id=(lat, 0),
            device_id_type=MESH,
        )

    @pl.when(lon == 0)
    def _():
        for other in range(lons - 1, 0, -1):
            head_copy(other).start()

    for other in range(devices):

        @pl.when(me != other)
        def _():
            stat_copy(me, 1, other).start()

    pl.when(jnp.logical_not(soon))(compact_ends)

    @pl.when(lon < lons - 1)
    def _():
        near_copy(1, 0, lon + 1).start()

    @pl.when(lon > 0)
    def _():
        near_copy(0, 1, lon - 1).start()
        tail_copy(lon).start()

    lax.fori_loop(bands_before, bands, spread_band, 0)
    lax.fori_loop(pairs_before, bands // PAIR, own_part, 0)

    def early(chosen, extras, block, offset):
        made = []
        low_e = iota(extras[0].shape, 1) < K
        skip = 2 * ends - extras[0].shape[0]
        for extra in extras:
            swapped = pltpu.roll(extra, K, 1)
            made.append(half_gram(jnp.where(low_e, extra, swapped)))
            made.append(half_gram(jnp.where(low_e, swapped, extra)))
        places = [(j, j * groups + g) for j in range(bands) for g in chosen]

        def column_group(line, j, i):
            gram = c_own[i] + dot(made[j][0], weighted(made[j][1], w_side[i, skip:]))
            yield
            c = gram[:K]
            c_out[i] = c
            narrow = c.astype(BF16)
            mean = gram[K : K + 1]
            old = x_out[i]
            middle = jnp.where(row_id == spare, mean, old[16:32].astype(F32)).astype(BF16)
            field = jnp.concatenate([old[:16], middle, old[32:]], axis=0)
            x_out[i] = field
            norm[block, 0, line : line + 1, :] = jnp.sum(c * c, axis=0, keepdims=True)
            norm[block, 1, line : line + 1, :] = jnp.sum(c * eye, axis=0, keepdims=True)
            both = dot(jnp.concatenate([narrow, field], axis=0), block_diag(narrow))
            yield
            s_out[i] = both[:K]
            p_out[i] = both[K:]
            cube = dot(narrow, block_diag(both[:K].astype(BF16)))
            yield
            q_out[i] = cube

        return [column_group(offset + n, j, i) for n, (j, i) in enumerate(places)]

    @pl.when(lon > 0)
    def _():
        head_copy(lon).wait_recv()

    halves = bands // PAIR
    centre_groups = range(edge, groups - edge)
    heads = [near_buf[2, p].astype(F32) for p in range(halves)]
    wavefront(early(centre_groups, heads, 0, 0), GAP_EARLY)

    def settle(block, shift, sums):
        inv = lax.rsqrt(sums[0] + shift * (2.0 * sums[1] + K * shift))
        scaling = jnp.sqrt((K - 1.0) * inv)
        beta = 1.0 - shift * inv
        beta1 = beta * beta * (0.75 + 0.25 * beta)
        beta2 = beta1 * beta1 * (0.75 + 0.25 * beta1)
        a0 = 1.0 + 0.5 * beta
        a1 = 1.0 + 0.5 * beta1
        half1 = 0.5 / a1
        c0 = (1.0 + 0.5 * beta2) * (1.0 + (0.375 + 0.125 * beta2) * beta2 * beta2)
        c1 = 0.5 + beta2 * (0.75 + beta2 * (0.9375 + 0.25 * beta2))
        c2 = 0.375 + beta2 * (0.9375 + 0.375 * beta2)
        c3 = 0.3125 + 0.25 * beta2
        up, down = c1 / c0, c0 / c1
        whole = a0 * a1 * c0
        table = (
            -inv * (1.5 * beta + 0.75 * beta * beta) * half1,
            inv * inv * (0.75 + 0.75 * beta) * half1,
            -0.25 * inv * inv * inv * half1,
            -0.5 * inv / a0,
            2.0 * a1 * up * (1.5 * beta1 + 0.75 * beta1 * beta1),
            4.0 * a1 * a1 * up * (0.75 + 0.75 * beta1),
            2.0 * a1 * a1 * a1 * up,
            c2 / c0 * down * down,
            c3 / c0 * down * down * down,
            0.0625 / c0 * (down * down) * (down * down),
            whole * whole * inv,
            (1.0 - scaling * whole) * (1.0 / K),
            scaling * whole,
        )
        for t, value in enumerate(table):
            coef[block, t] = value

    def finish(work):
        def k(t, w):
            return coef[w[0], t, w[1] : w[1] + 1, :]

        def wide_x(w):
            return x_out[w[2]].astype(F32)

        held = {}

        def column_group(n, w):
            i = w[2]
            m = k(0, w) * c_out[i] + k(1, w) * s_out[i] + k(2, w) * q_out[i]
            x = wide_x(w) + k(3, w) * p_out[i]
            m_b = m.astype(BF16)
            both = dot(jnp.concatenate([m_b, x.astype(BF16)], axis=0), block_diag(m_b))
            yield
            square = both[:K]
            cube = dot(m_b, block_diag(square.astype(BF16)))
            x = x + both[K:]
            yield
            m_b = (k(4, w) * m + k(5, w) * square + k(6, w) * cube).astype(BF16)
            x_b = x.astype(BF16)
            both = dot(jnp.concatenate([m_b, x_b], axis=0), block_diag(m_b))
            yield
            fixed = block_diag(both[:K].astype(BF16))
            quad = dot(x_b, fixed)
            part = k(7, w) * x + k(8, w) * both[K:]
            x = x + both[K:]
            yield
            last = dot((part + k(9, w) * quad).astype(BF16), fixed)
            yield
            x = x + last
            step = x[spare : spare + 1] * k(10, w)
            held[n] = (x * step + wide_x(w) * k(11, w)).astype(BF16)
            if n % SHARED == SHARED - 1 or n + 1 == len(work):
                first_n = n - n % SHARED
                stack = jnp.concatenate([held[v] for v in range(first_n, n + 1)], axis=0)
                means = dot(stack, ones_bd)
                rows = stack.shape[0] // (n + 1 - first_n)
                for v in range(first_n, n + 1):
                    held[v] = means[(v - first_n) * rows : (v - first_n + 1) * rows]
            yield
            yield
            result = k(12, w) * x + held[n]
            b, g = i // groups, i % groups
            for side in range(2):
                c = g * GROUP + 2 * side
                got = result[:, side * LANES : (side + 1) * LANES]
                evens, odds = got[:rows_x], got[rows_x:]
                r_out[b, c * rows_x : (c + 1) * rows_x, :] = jnp.where(
                    low_x, evens, pltpu.roll(odds, K, 1)
                )
                r_out[b, (c + 1) * rows_x : (c + 2) * rows_x, :] = jnp.where(
                    low_x, pltpu.roll(evens, K, 1), odds
                )

        return [column_group(n, w) for n, w in enumerate(work)]

    def lines(block, offset, chosen):
        places = [b * groups + g for b in range(bands) for g in chosen]
        return [(block, offset + n, i) for n, i in enumerate(places)]

    ones_bd = block_diag(jnp.ones((K, SPAN), BF16))

    def block_sums(block):
        both = jnp.concatenate([norm[block, 0], norm[block, 1]], axis=0)
        coarse = both.astype(BF16)
        fine = (both - coarse.astype(F32)).astype(BF16)
        size = both.shape[0]
        sums = dot(jnp.concatenate([coarse, fine], axis=0), ones_bd)
        sums = sums[:size] + sums[size:]
        return sums[: size // 2], sums[size // 2 :]

    first_sums = block_sums(0)
    everyone = stat_copy(0, devices - 1, 0)
    everyone.wait_send()
    everyone.wait_recv()
    stats = jnp.sum(stat_buf[...], axis=0)
    inflation = (stats[:, 0:1] + 1e-06) / stats[:, 1:2]
    shift = (K - 1) / inflation
    line = iota((8, LANES), 0)
    info = jnp.zeros((8, LANES), F32)
    for b in range(bands):
        info = jnp.where(line == b, (cols_ref[b] - first).astype(F32), info)
    info_out[...] = info
    settle(0, shift, first_sums)
    wavefront(finish(lines(0, 0, centre_groups)), GAP_LATE)

    @pl.when(lon < lons - 1)
    def _():
        near_copy(0, 1, lon + 1).wait_recv()

    @pl.when(lon > 0)
    def _():
        near_copy(1, 0, lon - 1).wait_recv()

    @pl.when(lon == 0)
    def _():
        pltpu.make_async_remote_copy(
            src_ref=tail_buf.at[pl.ds(1, lons - 1)],
            dst_ref=tail_buf.at[pl.ds(1, lons - 1)],
            send_sem=tail_send,
            recv_sem=tail_recv,
            device_id=(lat, 0),
            device_id_type=MESH,
        ).wait_recv()

    lefts, rights = [], []
    for p in range(halves):
        ahead = near_buf[0, p].astype(F32)
        for other in range(1, lons):
            ahead = ahead + tail_buf[other, p].astype(F32)
        lefts.append(jnp.concatenate([ahead, heads[p]], axis=0))
        rights.append(jnp.concatenate([near_buf[1, p].astype(F32), heads[p]], axis=0))
    left_groups, right_groups = range(edge), range(groups - edge, groups)
    wavefront(
        early(right_groups, rights, 1, 0) + early(left_groups, lefts, 1, bands * edge), GAP_EARLY
    )
    settle(1, shift, block_sums(1))
    wavefront(
        finish(lines(1, 0, right_groups) + lines(1, bands * edge, left_groups)), GAP_LATE
    )

    @pl.when(lon > 0)
    def _():
        tail_copy(lon).wait_send()
        near_copy(0, 1, lon - 1).wait_send()

    @pl.when(lon == 0)
    def _():
        for other in range(1, lons):
            head_copy(other).wait_send()

    @pl.when(lon < lons - 1)
    def _():
        near_copy(1, 0, lon + 1).wait_send()


def layout_kernel(r_ref, info_ref, out_hbm, obuf, out_sem):
    bands, columns, width = obuf.shape
    pairs = width // LANES
    rows_x = r_ref.shape[1] // columns

    def write(b):
        return pltpu.make_async_copy(obuf.at[b], out_hbm.at[b], out_sem.at[b])

    for b in range(bands):
        keep = iota((columns, LANES), 0).astype(F32) < info_ref[b : b + 1, :]
        for t in range(pairs):
            obuf[b, :, t * LANES : (t + 1) * LANES] = jnp.where(
                keep, r_ref[b, pl.ds(t, columns, stride=rows_x), :], 0.0
            ).astype(BF16)
        write(b).start()
    for b in range(bands):
        write(b).wait()


def per_device(lats, lons, background, band_cols, obs_col, obs_lev, obs_mask, innov, obs_var):
    bands, columns, width = background.shape
    obs = obs_col.shape[1]
    pairs = width // LANES
    devices = lats * lons
    vmem = pl.BlockSpec(memory_space=pltpu.VMEM)
    hbm = pl.BlockSpec(memory_space=pltpu.HBM)
    dma = pltpu.SemaphoreType.DMA
    rows_x = -(-(pairs + 1) // 8) * 8
    halves = bands // PAIR
    slots = obs + 2 * END_SLOTS
    total = bands * columns // GROUP
    rim = 2 * -(-(RADIUS - 1) // GROUP) * bands
    most = -(-max(rim, total - rim) // 8) * 8
    room = 16 * 1024 * 1024
    arrays = (background, obs_col, obs_lev, obs_mask, innov, obs_var, band_cols)
    groups_f32 = pltpu.VMEM((total, K, SPAN), F32)
    result, info = pl.pallas_call(
        functools.partial(exchange_kernel, lats, lons),
        out_shape=(
            jax.ShapeDtypeStruct((bands, columns * rows_x, LANES), F32),
            jax.ShapeDtypeStruct((8, LANES), F32),
        ),
        in_specs=[hbm] * 7,
        out_specs=(vmem,) * 2,
        scratch_shapes=[
            groups_f32,
            groups_f32,
            groups_f32,
            pltpu.VMEM((total, 2 * rows_x, SPAN), F32),
            pltpu.VMEM((total, 2 * rows_x, SPAN), BF16),
            pltpu.VMEM((2, 2, most, SPAN), F32),
            pltpu.VMEM((2, 13, most, SPAN), F32),
            pltpu.VMEM((bands, columns, width), BF16),
            pltpu.VMEM((bands, obs), jnp.int32),
            pltpu.VMEM((bands, obs), jnp.int32),
            pltpu.VMEM((bands, obs), jnp.int32),
            pltpu.VMEM((bands, obs), F32),
            pltpu.VMEM((bands, obs), F32),
            pltpu.SMEM((bands,), jnp.int32),
            pltpu.VMEM((columns * rows_x, LANES), F32),
            pltpu.VMEM((bands * obs, LANES), F32),
            pltpu.VMEM((2, slots, LANES), BF16),
            pltpu.VMEM((total, 2 * END_SLOTS, SPAN), F32),
            pltpu.VMEM((total, K + 16, SPAN), F32),
            pltpu.VMEM((3, halves, END_SLOTS, LANES), BF16),
            pltpu.VMEM((3, halves, END_SLOTS, LANES), BF16),
            pltpu.VMEM((lons, halves, END_SLOTS, LANES), BF16),
            pltpu.VMEM((devices, 1, LANES), F32),
            dma((bands,)),
            dma((6,)),
            dma((2,)),
            dma((2,)),
            dma((lons,)),
            dma,
            dma,
            dma,
            dma,
            dma,
        ],
        compiler_params=pltpu.CompilerParams(
            collective_id=0, has_side_effects=True, vmem_limit_bytes=2 * room
        ),
        name="exchange",
    )(*(pltpu.with_memory_space_constraint(a, pltpu.HBM) for a in arrays))
    return pl.pallas_call(
        layout_kernel,
        out_shape=jax.ShapeDtypeStruct(background.shape, BF16),
        in_specs=[vmem] * 2,
        out_specs=hbm,
        scratch_shapes=[
            pltpu.VMEM((bands, columns, width), BF16),
            dma((bands,)),
        ],
        compiler_params=pltpu.CompilerParams(vmem_limit_bytes=room),
        name="layout",
    )(result, info)


def solution(mesh):
    placed = (P("lat", "lon", None), P("lat")) + (P("lat", "lon"),) * 5
    return jax.shard_map(
        functools.partial(per_device, mesh.shape["lat"], mesh.shape["lon"]),
        mesh=mesh,
        in_specs=placed,
        out_specs=P("lat", "lon", None),
        check_vma=False,
    )
```

```python
import functools

import jax
import jax.numpy as jnp
from jax import lax
from jax.experimental import pallas as pl
from jax.experimental.pallas import tpu as pltpu
from jax.sharding import PartitionSpec as P

K = 64
RADIUS = 8
GROUP = 4
OC = 4
END_SLOTS = 32
FAR = 1 << 20
GAP_OWN = 16
GAP_EARLY = 12
GAP_LATE = 8
SHARED = 4
LANES = 128
PAIR = 2
SPAN = GROUP * K
F32 = jnp.float32
BF16 = jnp.bfloat16
MESH = pl.DeviceIdType.MESH


def taper_weights(radius):
    half_width = radius / 2.0
    tapering = []
    for offset in range(radius):
        distance = offset / half_width
        if distance <= 1.0:
            weight = (
                ((-0.25 * distance + 0.5) * distance + 0.625) * distance**3
                - 5.0 / 3.0 * distance**2
                + 1.0
            )
        else:
            weight = (
                (((distance / 12.0 - 0.5) * distance + 0.625) * distance + 5.0 / 3.0) * distance**2
                - 5.0 * distance
                + 4.0
                - 2.0 / (3.0 * distance)
            )
        tapering.append(weight)
    return tapering


def dot(left, right):
    return jnp.dot(left, right, preferred_element_type=F32)


def iota(shape, dim):
    return lax.broadcasted_iota(jnp.int32, shape, dim)


def block_diag(mat):
    lanes = iota((K, LANES), 1)
    zero = jnp.zeros((K, LANES), BF16)
    left, right = mat[:, :LANES], mat[:, LANES:]
    return jnp.concatenate(
        [
            jnp.concatenate([jnp.where(lanes < K, left, zero), zero], axis=1),
            jnp.concatenate([jnp.where(lanes < K, zero, left), zero], axis=1),
            jnp.concatenate([zero, jnp.where(lanes < K, right, zero)], axis=1),
            jnp.concatenate([zero, jnp.where(lanes < K, zero, right)], axis=1),
        ],
        axis=0,
    )


def wavefront(tasks, gap):
    started = []
    step = 0
    while step < len(tasks) or started:
        if step < len(tasks):
            started.append((step, tasks[step]))
        left = []
        for begin, task in started:
            if (step - begin) % gap == 0:
                try:
                    next(task)
                except StopIteration:
                    continue
            left.append((begin, task))
        started = left
        step += 1


def exchange_kernel(
    lats,
    lons,
    x_hbm,
    col_hbm,
    lev_hbm,
    mask_hbm,
    innov_hbm,
    var_hbm,
    cols_hbm,
    r_out,
    info_out,
    c_out,
    s_out,
    q_out,
    p_out,
    x_out,
    norm,
    coef,
    x_v,
    col_ref,
    lev_ref,
    mask_ref,
    innov_ref,
    var_ref,
    cols_ref,
    xs,
    own,
    weights,
    w_side,
    c_own,
    ends_buf,
    near_buf,
    tail_buf,
    stat_buf,
    x_sem,
    in_sem,
    near_send,
    near_recv,
    head_send,
    head_recv,
    tail_send,
    tail_recv,
    stat_send,
    stat_recv,
):
    lat, lon = lax.axis_index("lat"), lax.axis_index("lon")
    bands, columns, width = x_v.shape
    obs = col_ref.shape[1]
    devices = lats * lons
    me = lat * lons + lon
    smalls = (
        (col_hbm, col_ref),
        (lev_hbm, lev_ref),
        (mask_hbm, mask_ref),
        (innov_hbm, innov_ref),
        (var_hbm, var_ref),
        (cols_hbm, cols_ref),
    )
    loads = [
        pltpu.make_async_copy(source, target, in_sem.at[i])
        for i, (source, target) in enumerate(smalls)
    ]
    x_loads = [pltpu.make_async_copy(x_hbm.at[b], x_v.at[b], x_sem.at[b]) for b in range(bands)]
    for load in loads + x_loads:
        load.start()
    barrier = pltpu.get_barrier_semaphore()
    near_buf[...] = jnp.zeros_like(near_buf)
    tail_buf[...] = jnp.zeros_like(tail_buf)

    for other in range(devices):

        @pl.when(me != other)
        def _():
            pl.semaphore_signal(
                barrier, inc=1, device_id=(other // lons, other % lons), device_id_type=MESH
            )

    xs[...] = jnp.zeros_like(xs)
    norm[...] = jnp.zeros_like(norm)
    pairs = width // LANES
    reach = RADIUS - 1
    ends = END_SLOTS
    first = lon * columns
    for load in loads:
        load.wait()
    mask = mask_ref[...].astype(F32)
    used_all = mask > 0.0
    local_int = jnp.where(used_all, col_ref[...] - first, -columns)
    local = local_int.astype(F32)
    lev = lev_ref[...]
    spot = (lax.shift_right_logical(lev, 1) * columns + col_ref[...] - first) * 2 + (lev & 1)
    scale = jnp.sqrt(mask / var_ref[...])
    params = jnp.concatenate([local, spot.astype(F32), scale, innov_ref[...]], axis=0)
    params = jnp.concatenate([params, jnp.zeros((LANES - 4 * bands, obs), F32)], axis=0)
    params = jnp.concatenate([params, jnp.zeros((LANES, LANES - obs), F32)], axis=1)
    upright = jnp.transpose(params)[:obs]
    earlier = iota((obs, obs), 0) < iota((obs, obs), 1)
    slot_ids = iota((ends, obs), 0)

    def stacked(kind):
        return jnp.concatenate(
            [upright[:, kind * bands + b : kind * bands + b + 1] for b in range(bands)], axis=0
        )

    marks = []
    for b in range(bands):
        row = local_int[b : b + 1]
        used = used_all[b : b + 1]
        same = (upright[:, b : b + 1] == local[b : b + 1]) & earlier
        rank = jnp.sum(jnp.where(same, 1.0, 0.0), axis=0, keepdims=True).astype(jnp.int32)
        bases = (row, row - (columns - reach), row + first - (cols_ref[b] - reach))
        mark = []
        for base in bases:
            fits = used & (base >= 0) & (base < reach)
            slot = jnp.where(fits, base * OC + rank, -1)
            mark.append(jnp.where(slot_ids == slot, 1.0, 0.0))
        marks.append(jnp.concatenate(mark, axis=0).astype(BF16))

    tapering = taper_weights(RADIUS)
    lane = iota((1, LANES), 1)
    lane_band, lane_col = lane // columns, lane % columns
    count = jnp.zeros((1, LANES), jnp.int32)
    for b in range(bands):
        count = jnp.where(lane_band == b, cols_ref[b], count)
    chooser = jnp.where(iota((LANES, LANES), 0) == lane_band, 1.0, 0.0).astype(BF16)
    source = dot(upright.astype(BF16), chooser).astype(jnp.int32)
    nth = iota((ends, LANES), 0) // OC

    def taper(place, limit):
        away = place - lane_col
        away = jnp.where(2 * away > limit, away - limit, away)
        away = jnp.where(2 * away < -limit, away + limit, away)
        away = jnp.abs(away)
        weight = jnp.zeros(place.shape, F32)
        for t in range(RADIUS):
            weight = jnp.where(away == t, tapering[t], weight)
        return weight.astype(BF16)

    near_own = taper(source, count)
    near_left = taper(nth - reach, FAR)
    near_right = taper(nth + columns, FAR)
    near_head = taper(nth + count - first, FAR)
    beside = (
        jnp.concatenate([near_right, near_head], axis=0),
        jnp.concatenate([near_left, near_head], axis=0),
    )
    weights[0] = jnp.concatenate([near_own, beside[0]], axis=0)
    weights[1] = jnp.concatenate([near_own, beside[1]], axis=0)

    spots = stacked(1).astype(jnp.int32)
    scales = stacked(2)
    depth = pairs * columns
    gathered = []
    for b in range(bands):
        index = lax.shift_right_logical(spots[b * obs : (b + 1) * obs], 1)
        onehot = jnp.where(iota((obs, depth), 1) == index, 1.0, 0.0).astype(BF16)
        x_loads[b].wait()
        field = jnp.concatenate(
            [x_v[b, :, p * LANES : (p + 1) * LANES] for p in range(pairs)], axis=0
        )
        gathered.append(dot(onehot, field))
    found = jnp.concatenate(gathered, axis=0)
    total = bands * obs
    low_t = iota((total, LANES), 1) < K
    even = (spots & 1) == 0
    picked = jnp.where(low_t == even, found, pltpu.roll(found, K, 1))
    anomaly = picked - jnp.mean(picked, axis=1, keepdims=True)
    departs = (scales * (anomaly - stacked(3))).astype(BF16)
    wide = departs.astype(F32)
    own[...] = wide
    centre = jnp.mean(wide, axis=1, keepdims=True)
    spread = wide - centre
    numerator = jnp.sum(centre * centre, axis=0, keepdims=True)
    spread_row = jnp.sum(spread * spread, axis=0, keepdims=True)
    mask_row = jnp.sum(mask, axis=0, keepdims=True)
    denominator = jnp.sum(spread_row, axis=1, keepdims=True) * (0.5 / (K - 1)) + jnp.sum(
        mask_row, axis=1, keepdims=True
    )
    stat_buf[me] = jnp.where(iota((1, LANES), 1) == 0, numerator, denominator)

    def compact_ends():
        low = iota((obs, LANES), 1) < K
        for q in range(bands // PAIR):
            mark = jnp.concatenate([marks[2 * q], marks[2 * q + 1]], axis=1)
            one = wide[(2 * q) * obs : (2 * q + 1) * obs]
            two = wide[(2 * q + 1) * obs : (2 * q + 2) * obs]
            both = jnp.concatenate(
                [jnp.where(low, one, 0.0), jnp.where(low, 0.0, two)], axis=0
            ).astype(BF16)
            compact = dot(mark, both).astype(BF16)
            for kind in range(3):
                ends_buf[kind, q] = compact[kind * ends : (kind + 1) * ends]

    soon = lon < lons // 2
    pl.when(soon)(compact_ends)

    rows_x = xs.shape[0] // columns
    groups = columns // GROUP
    low_x = iota((rows_x, LANES), 1) < K
    def spread_band(b, carry):
        for p in range(pairs):
            strip = x_v[b, :, p * LANES : (p + 1) * LANES].astype(F32)
            xs[pl.ds(p, columns, stride=rows_x), :] = strip
        for g in range(groups):
            halves = []
            for c in (g * GROUP, g * GROUP + 2):
                here = xs[c * rows_x : (c + 1) * rows_x, :]
                there = xs[(c + 1) * rows_x : (c + 2) * rows_x, :]
                halves.append(
                    jnp.concatenate(
                        [
                            jnp.where(low_x, here, pltpu.roll(there, K, 1)),
                            jnp.where(low_x, pltpu.roll(here, K, 1), there),
                        ],
                        axis=0,
                    ).astype(BF16)
                )
            x_out[b * groups + g] = jnp.concatenate(halves, axis=1)
        return carry

    eye = jnp.where(iota((K, SPAN), 0) == iota((K, SPAN), 1) % K, 1.0, 0.0)
    spare = pairs
    expand_row = iota((LANES, SPAN), 0) - iota((LANES, SPAN), 1) // K
    row_id = iota((16, SPAN), 0) + 16

    edge = -(-reach // GROUP)

    def half_gram(slot):
        spread = slot - jnp.mean(slot, axis=1, keepdims=True)
        rows = slot.shape[0]
        square = jnp.concatenate([slot, jnp.zeros((LANES - rows, LANES), F32)], axis=0)
        turned = jnp.transpose(square)[:K, :rows]
        centre = jnp.mean(turned, axis=0, keepdims=True)
        left = jnp.concatenate([turned - centre, -centre, jnp.zeros((15, rows), F32)], axis=0)
        return left.astype(BF16), spread

    def weighted(spread, wide_w):
        return jnp.concatenate(
            [
                (spread * wide_w[:, :LANES]).astype(BF16),
                (spread * wide_w[:, LANES:]).astype(BF16),
            ],
            axis=1,
        )

    def own_part(p, carry):
        made = []
        for j in range(PAIR):
            start = pl.multiple_of((p * PAIR + j) * obs, obs)
            made.append(half_gram(own[pl.ds(start, obs), :]))

        def column_group(j, g):
            i = (p * PAIR + j) * groups + g
            picker = jnp.where(
                expand_row == (p * PAIR + j) * columns + g * GROUP, 1.0, 0.0
            ).astype(BF16)
            wide_w = dot(weights[1 if g < edge else 0], picker)
            yield
            w_side[i] = wide_w[obs:]
            gram = dot(made[j][0], weighted(made[j][1], wide_w[:obs]))
            yield
            c_own[i] = gram

        wavefront([column_group(j, g) for j in range(PAIR) for g in range(groups)], GAP_OWN)
        return carry

    bands_before = jnp.where(soon, bands, 0)
    pairs_before = jnp.where(soon, bands // PAIR, 0)
    lax.fori_loop(0, bands_before, spread_band, 0)
    lax.fori_loop(0, pairs_before, own_part, 0)

    pl.semaphore_wait(barrier, devices - 1)

    def stat_copy(slot, size, other):
        return pltpu.make_async_remote_copy(
            src_ref=stat_buf.at[pl.ds(slot, size)],
            dst_ref=stat_buf.at[pl.ds(slot, size)],
            send_sem=stat_send,
            recv_sem=stat_recv,
            device_id=(other // lons, other % lons),
            device_id_type=MESH,
        )

    def near_copy(kind, slot, other):
        return pltpu.make_async_remote_copy(
            src_ref=ends_buf.at[kind],
            dst_ref=near_buf.at[slot],
            send_sem=near_send.at[slot],
            recv_sem=near_recv.at[slot],
            device_id=(lat, other),
            device_id_type=MESH,
        )

    def head_copy(other):
        return pltpu.make_async_remote_copy(
            src_ref=ends_buf.at[0],
            dst_ref=near_buf.at[2],
            send_sem=head_send.at[other],
            recv_sem=head_recv,
            device_id=(lat, other),
            device_id_type=MESH,
        )

    def tail_copy(slot):
        return pltpu.make_async_remote_copy(
            src_ref=ends_buf.at[2],
            dst_ref=tail_buf.at[slot],
            send_sem=tail_send,
            recv_sem=tail_recv,
            device_id=(lat, 0),
            device_id_type=MESH,
        )

    @pl.when(lon == 0)
    def _():
        for other in [*range(2, lons), 1]:
            head_copy(other).start()

    for other in range(devices):

        @pl.when(me != other)
        def _():
            stat_copy(me, 1, other).start()

    pl.when(jnp.logical_not(soon))(compact_ends)

    @pl.when(lon < lons - 1)
    def _():
        near_copy(1, 0, lon + 1).start()

    @pl.when(lon > 0)
    def _():
        near_copy(0, 1, lon - 1).start()
        tail_copy(lon).start()

    lax.fori_loop(bands_before, bands, spread_band, 0)
    lax.fori_loop(pairs_before, bands // PAIR, own_part, 0)

    def early(chosen, extras, block, offset):
        made = []
        low_e = iota(extras[0].shape, 1) < K
        skip = 2 * ends - extras[0].shape[0]
        for extra in extras:
            swapped = pltpu.roll(extra, K, 1)
            made.append(half_gram(jnp.where(low_e, extra, swapped)))
            made.append(half_gram(jnp.where(low_e, swapped, extra)))
        places = [(j, j * groups + g) for j in range(bands) for g in chosen]

        def column_group(line, j, i):
            gram = c_own[i] + dot(made[j][0], weighted(made[j][1], w_side[i, skip:]))
            yield
            c = gram[:K]
            c_out[i] = c
            narrow = c.astype(BF16)
            mean = gram[K : K + 1]
            old = x_out[i]
            middle = jnp.where(row_id == spare, mean, old[16:32].astype(F32)).astype(BF16)
            field = jnp.concatenate([old[:16], middle, old[32:]], axis=0)
            x_out[i] = field
            norm[block, 0, line : line + 1, :] = jnp.sum(c * c, axis=0, keepdims=True)
            norm[block, 1, line : line + 1, :] = jnp.sum(c * eye, axis=0, keepdims=True)
            both = dot(jnp.concatenate([narrow, field], axis=0), block_diag(narrow))
            yield
            s_out[i] = both[:K]
            p_out[i] = both[K:]
            cube = dot(narrow, block_diag(both[:K].astype(BF16)))
            yield
            q_out[i] = cube

        return [column_group(offset + n, j, i) for n, (j, i) in enumerate(places)]

    @pl.when(lon > 0)
    def _():
        head_copy(lon).wait_recv()

    halves = bands // PAIR
    centre_groups = range(edge, groups - edge)
    heads = [near_buf[2, p].astype(F32) for p in range(halves)]
    wavefront(early(centre_groups, heads, 0, 0), GAP_EARLY)

    @pl.when(lon < lons - 1)
    def _():
        near_copy(0, 1, lon + 1).wait_recv()

    rights = [
        jnp.concatenate([near_buf[1, p].astype(F32), heads[p]], axis=0) for p in range(halves)
    ]
    left_groups, right_groups = range(edge), range(groups - edge, groups)
    wavefront(early(right_groups, rights, 1, 0), GAP_EARLY)

    def settle(block, shift, sums):
        inv = lax.rsqrt(sums[0] + shift * (2.0 * sums[1] + K * shift))
        scaling = jnp.sqrt((K - 1.0) * inv)
        beta = 1.0 - shift * inv
        beta1 = beta * beta * (0.75 + 0.25 * beta)
        beta2 = beta1 * beta1 * (0.75 + 0.25 * beta1)
        a0 = 1.0 + 0.5 * beta
        a1 = 1.0 + 0.5 * beta1
        half1 = 0.5 / a1
        c0 = (1.0 + 0.5 * beta2) * (1.0 + (0.375 + 0.125 * beta2) * beta2 * beta2)
        c1 = 0.5 + beta2 * (0.75 + beta2 * (0.9375 + 0.25 * beta2))
        c2 = 0.375 + beta2 * (0.9375 + 0.375 * beta2)
        c3 = 0.3125 + 0.25 * beta2
        up, down = c1 / c0, c0 / c1
        whole = a0 * a1 * c0
        table = (
            -inv * (1.5 * beta + 0.75 * beta * beta) * half1,
            inv * inv * (0.75 + 0.75 * beta) * half1,
            -0.25 * inv * inv * inv * half1,
            -0.5 * inv / a0,
            2.0 * a1 * up * (1.5 * beta1 + 0.75 * beta1 * beta1),
            4.0 * a1 * a1 * up * (0.75 + 0.75 * beta1),
            2.0 * a1 * a1 * a1 * up,
            c2 / c0 * down * down,
            c3 / c0 * down * down * down,
            0.0625 / c0 * (down * down) * (down * down),
            whole * whole * inv,
            (1.0 - scaling * whole) * (1.0 / K),
            scaling * whole,
        )
        for t, value in enumerate(table):
            coef[block, t] = value

    def finish(work):
        def k(t, w):
            return coef[w[0], t, w[1] : w[1] + 1, :]

        def wide_x(w):
            return x_out[w[2]].astype(F32)

        held = {}

        def column_group(n, w):
            i = w[2]
            m = k(0, w) * c_out[i] + k(1, w) * s_out[i] + k(2, w) * q_out[i]
            x = wide_x(w) + k(3, w) * p_out[i]
            m_b = m.astype(BF16)
            both = dot(jnp.concatenate([m_b, x.astype(BF16)], axis=0), block_diag(m_b))
            yield
            square = both[:K]
            cube = dot(m_b, block_diag(square.astype(BF16)))
            x = x + both[K:]
            yield
            m_b = (k(4, w) * m + k(5, w) * square + k(6, w) * cube).astype(BF16)
            x_b = x.astype(BF16)
            both = dot(jnp.concatenate([m_b, x_b], axis=0), block_diag(m_b))
            yield
            fixed = block_diag(both[:K].astype(BF16))
            quad = dot(x_b, fixed)
            part = k(7, w) * x + k(8, w) * both[K:]
            x = x + both[K:]
            yield
            last = dot((part + k(9, w) * quad).astype(BF16), fixed)
            yield
            x = x + last
            step = x[spare : spare + 1] * k(10, w)
            held[n] = (x * step + wide_x(w) * k(11, w)).astype(BF16)
            if n % SHARED == SHARED - 1 or n + 1 == len(work):
                first_n = n - n % SHARED
                stack = jnp.concatenate([held[v] for v in range(first_n, n + 1)], axis=0)
                means = dot(stack, ones_bd)
                rows = stack.shape[0] // (n + 1 - first_n)
                for v in range(first_n, n + 1):
                    held[v] = means[(v - first_n) * rows : (v - first_n + 1) * rows]
            yield
            yield
            result = k(12, w) * x + held[n]
            b, g = i // groups, i % groups
            for side in range(2):
                c = g * GROUP + 2 * side
                got = result[:, side * LANES : (side + 1) * LANES]
                evens, odds = got[:rows_x], got[rows_x:]
                r_out[b, c * rows_x : (c + 1) * rows_x, :] = jnp.where(
                    low_x, evens, pltpu.roll(odds, K, 1)
                )
                r_out[b, (c + 1) * rows_x : (c + 2) * rows_x, :] = jnp.where(
                    low_x, pltpu.roll(evens, K, 1), odds
                )

        return [column_group(n, w) for n, w in enumerate(work)]

    def lines(block, offset, chosen):
        places = [b * groups + g for b in range(bands) for g in chosen]
        return [(block, offset + n, i) for n, i in enumerate(places)]

    ones_bd = block_diag(jnp.ones((K, SPAN), BF16))

    def block_sums(block):
        both = jnp.concatenate([norm[block, 0], norm[block, 1]], axis=0)
        coarse = both.astype(BF16)
        fine = (both - coarse.astype(F32)).astype(BF16)
        size = both.shape[0]
        sums = dot(jnp.concatenate([coarse, fine], axis=0), ones_bd)
        sums = sums[:size] + sums[size:]
        return sums[: size // 2], sums[size // 2 :]

    first_sums = block_sums(0)
    everyone = stat_copy(0, devices - 1, 0)
    everyone.wait_send()
    everyone.wait_recv()
    stats = jnp.sum(stat_buf[...], axis=0)
    inflation = (stats[:, 0:1] + 1e-06) / stats[:, 1:2]
    shift = (K - 1) / inflation
    line = iota((8, LANES), 0)
    info = jnp.zeros((8, LANES), F32)
    for b in range(bands):
        info = jnp.where(line == b, (cols_ref[b] - first).astype(F32), info)
    info_out[...] = info
    settle(0, shift, first_sums)
    wavefront(finish(lines(0, 0, centre_groups)), GAP_LATE)

    @pl.when(lon > 0)
    def _():
        near_copy(1, 0, lon - 1).wait_recv()

    @pl.when(lon == 0)
    def _():
        pltpu.make_async_remote_copy(
            src_ref=tail_buf.at[pl.ds(1, lons - 1)],
            dst_ref=tail_buf.at[pl.ds(1, lons - 1)],
            send_sem=tail_send,
            recv_sem=tail_recv,
            device_id=(lat, 0),
            device_id_type=MESH,
        ).wait_recv()

    lefts = []
    for p in range(halves):
        ahead = near_buf[0, p].astype(F32)
        for other in range(1, lons):
            ahead = ahead + tail_buf[other, p].astype(F32)
        lefts.append(jnp.concatenate([ahead, heads[p]], axis=0))
    wavefront(early(left_groups, lefts, 1, bands * edge), GAP_EARLY)
    settle(1, shift, block_sums(1))
    wavefront(
        finish(lines(1, 0, right_groups) + lines(1, bands * edge, left_groups)), GAP_LATE
    )

    @pl.when(lon > 0)
    def _():
        tail_copy(lon).wait_send()
        near_copy(0, 1, lon - 1).wait_send()

    @pl.when(lon == 0)
    def _():
        for other in range(1, lons):
            head_copy(other).wait_send()

    @pl.when(lon < lons - 1)
    def _():
        near_copy(1, 0, lon + 1).wait_send()


def layout_kernel(r_ref, info_ref, out_hbm, obuf, out_sem):
    bands, columns, width = obuf.shape
    pairs = width // LANES
    rows_x = r_ref.shape[1] // columns

    def write(b):
        return pltpu.make_async_copy(obuf.at[b], out_hbm.at[b], out_sem.at[b])

    for b in range(bands):
        keep = iota((columns, LANES), 0).astype(F32) < info_ref[b : b + 1, :]
        for t in range(pairs):
            obuf[b, :, t * LANES : (t + 1) * LANES] = jnp.where(
                keep, r_ref[b, pl.ds(t, columns, stride=rows_x), :], 0.0
            ).astype(BF16)
        write(b).start()
    for b in range(bands):
        write(b).wait()


def per_device(lats, lons, background, band_cols, obs_col, obs_lev, obs_mask, innov, obs_var):
    bands, columns, width = background.shape
    obs = obs_col.shape[1]
    pairs = width // LANES
    devices = lats * lons
    vmem = pl.BlockSpec(memory_space=pltpu.VMEM)
    hbm = pl.BlockSpec(memory_space=pltpu.HBM)
    dma = pltpu.SemaphoreType.DMA
    rows_x = -(-(pairs + 1) // 8) * 8
    halves = bands // PAIR
    slots = obs + 2 * END_SLOTS
    total = bands * columns // GROUP
    rim = 2 * -(-(RADIUS - 1) // GROUP) * bands
    most = -(-max(rim, total - rim) // 8) * 8
    room = 16 * 1024 * 1024
    arrays = (background, obs_col, obs_lev, obs_mask, innov, obs_var, band_cols)
    groups_f32 = pltpu.VMEM((total, K, SPAN), F32)
    result, info = pl.pallas_call(
        functools.partial(exchange_kernel, lats, lons),
        out_shape=(
            jax.ShapeDtypeStruct((bands, columns * rows_x, LANES), F32),
            jax.ShapeDtypeStruct((8, LANES), F32),
        ),
        in_specs=[hbm] * 7,
        out_specs=(vmem,) * 2,
        scratch_shapes=[
            groups_f32,
            groups_f32,
            groups_f32,
            pltpu.VMEM((total, 2 * rows_x, SPAN), F32),
            pltpu.VMEM((total, 2 * rows_x, SPAN), BF16),
            pltpu.VMEM((2, 2, most, SPAN), F32),
            pltpu.VMEM((2, 13, most, SPAN), F32),
            pltpu.VMEM((bands, columns, width), BF16),
            pltpu.VMEM((bands, obs), jnp.int32),
            pltpu.VMEM((bands, obs), jnp.int32),
            pltpu.VMEM((bands, obs), jnp.int32),
            pltpu.VMEM((bands, obs), F32),
            pltpu.VMEM((bands, obs), F32),
            pltpu.SMEM((bands,), jnp.int32),
            pltpu.VMEM((columns * rows_x, LANES), F32),
            pltpu.VMEM((bands * obs, LANES), F32),
            pltpu.VMEM((2, slots, LANES), BF16),
            pltpu.VMEM((total, 2 * END_SLOTS, SPAN), F32),
            pltpu.VMEM((total, K + 16, SPAN), F32),
            pltpu.VMEM((3, halves, END_SLOTS, LANES), BF16),
            pltpu.VMEM((3, halves, END_SLOTS, LANES), BF16),
            pltpu.VMEM((lons, halves, END_SLOTS, LANES), BF16),
            pltpu.VMEM((devices, 1, LANES), F32),
            dma((bands,)),
            dma((6,)),
            dma((2,)),
            dma((2,)),
            dma((lons,)),
            dma,
            dma,
            dma,
            dma,
            dma,
        ],
        compiler_params=pltpu.CompilerParams(
            collective_id=0, has_side_effects=True, vmem_limit_bytes=2 * room
        ),
        name="exchange",
    )(*(pltpu.with_memory_space_constraint(a, pltpu.HBM) for a in arrays))
    return pl.pallas_call(
        layout_kernel,
        out_shape=jax.ShapeDtypeStruct(background.shape, BF16),
        in_specs=[vmem] * 2,
        out_specs=hbm,
        scratch_shapes=[
            pltpu.VMEM((bands, columns, width), BF16),
            dma((bands,)),
        ],
        compiler_params=pltpu.CompilerParams(vmem_limit_bytes=room),
        name="layout",
    )(result, info)


def solution(mesh):
    placed = (P("lat", "lon", None), P("lat")) + (P("lat", "lon"),) * 5
    return jax.shard_map(
        functools.partial(per_device, mesh.shape["lat"], mesh.shape["lon"]),
        mesh=mesh,
        in_specs=placed,
        out_specs=P("lat", "lon", None),
        check_vma=False,
    )
```

```python
import functools

import jax
import jax.numpy as jnp
from jax import lax
from jax.experimental import pallas as pl
from jax.experimental.pallas import tpu as pltpu
from jax.sharding import PartitionSpec as P

K = 64
RADIUS = 8
GROUP = 4
OC = 4
END_SLOTS = 32
FAR = 1 << 20
GAP_OWN = 16
GAP_EARLY = 12
GAP_LATE = 8
SHARED = 8
LANES = 128
PAIR = 2
SPAN = GROUP * K
F32 = jnp.float32
BF16 = jnp.bfloat16
MESH = pl.DeviceIdType.MESH


def taper_weights(radius):
    half_width = radius / 2.0
    tapering = []
    for offset in range(radius):
        distance = offset / half_width
        if distance <= 1.0:
            weight = (
                ((-0.25 * distance + 0.5) * distance + 0.625) * distance**3
                - 5.0 / 3.0 * distance**2
                + 1.0
            )
        else:
            weight = (
                (((distance / 12.0 - 0.5) * distance + 0.625) * distance + 5.0 / 3.0) * distance**2
                - 5.0 * distance
                + 4.0
                - 2.0 / (3.0 * distance)
            )
        tapering.append(weight)
    return tapering


def dot(left, right):
    return jnp.dot(left, right, preferred_element_type=F32)


def iota(shape, dim):
    return lax.broadcasted_iota(jnp.int32, shape, dim)


def block_diag(mat):
    lanes = iota((K, LANES), 1)
    zero = jnp.zeros((K, LANES), BF16)
    left, right = mat[:, :LANES], mat[:, LANES:]
    return jnp.concatenate(
        [
            jnp.concatenate([jnp.where(lanes < K, left, zero), zero], axis=1),
            jnp.concatenate([jnp.where(lanes < K, zero, left), zero], axis=1),
            jnp.concatenate([zero, jnp.where(lanes < K, right, zero)], axis=1),
            jnp.concatenate([zero, jnp.where(lanes < K, zero, right)], axis=1),
        ],
        axis=0,
    )


def wavefront(tasks, gap):
    started = []
    step = 0
    while step < len(tasks) or started:
        if step < len(tasks):
            started.append((step, tasks[step]))
        left = []
        for begin, task in started:
            if (step - begin) % gap == 0:
                try:
                    next(task)
                except StopIteration:
                    continue
            left.append((begin, task))
        started = left
        step += 1


def exchange_kernel(
    lats,
    lons,
    x_hbm,
    col_hbm,
    lev_hbm,
    mask_hbm,
    innov_hbm,
    var_hbm,
    cols_hbm,
    r_out,
    info_out,
    c_out,
    s_out,
    q_out,
    p_out,
    x_out,
    norm,
    coef,
    x_v,
    col_ref,
    lev_ref,
    mask_ref,
    innov_ref,
    var_ref,
    cols_ref,
    xs,
    own,
    weights,
    w_side,
    c_own,
    ends_buf,
    near_buf,
    tail_buf,
    stat_buf,
    x_sem,
    in_sem,
    near_send,
    near_recv,
    head_send,
    head_recv,
    tail_send,
    tail_recv,
    stat_send,
    stat_recv,
):
    lat, lon = lax.axis_index("lat"), lax.axis_index("lon")
    bands, columns, width = x_v.shape
    obs = col_ref.shape[1]
    devices = lats * lons
    me = lat * lons + lon
    smalls = (
        (col_hbm, col_ref),
        (lev_hbm, lev_ref),
        (mask_hbm, mask_ref),
        (innov_hbm, innov_ref),
        (var_hbm, var_ref),
        (cols_hbm, cols_ref),
    )
    loads = [
        pltpu.make_async_copy(source, target, in_sem.at[i])
        for i, (source, target) in enumerate(smalls)
    ]
    x_loads = [pltpu.make_async_copy(x_hbm.at[b], x_v.at[b], x_sem.at[b]) for b in range(bands)]
    for load in loads + x_loads:
        load.start()
    barrier = pltpu.get_barrier_semaphore()
    near_buf[...] = jnp.zeros_like(near_buf)
    tail_buf[...] = jnp.zeros_like(tail_buf)

    for other in range(devices):

        @pl.when(me != other)
        def _():
            pl.semaphore_signal(
                barrier, inc=1, device_id=(other // lons, other % lons), device_id_type=MESH
            )

    xs[...] = jnp.zeros_like(xs)
    norm[...] = jnp.zeros_like(norm)
    pairs = width // LANES
    reach = RADIUS - 1
    ends = END_SLOTS
    first = lon * columns
    for load in loads:
        load.wait()
    mask = mask_ref[...].astype(F32)
    used_all = mask > 0.0
    local_int = jnp.where(used_all, col_ref[...] - first, -columns)
    local = local_int.astype(F32)
    lev = lev_ref[...]
    spot = (lax.shift_right_logical(lev, 1) * columns + col_ref[...] - first) * 2 + (lev & 1)
    scale = jnp.sqrt(mask / var_ref[...])
    params = jnp.concatenate([local, spot.astype(F32), scale, innov_ref[...]], axis=0)
    params = jnp.concatenate([params, jnp.zeros((LANES - 4 * bands, obs), F32)], axis=0)
    params = jnp.concatenate([params, jnp.zeros((LANES, LANES - obs), F32)], axis=1)
    upright = jnp.transpose(params)[:obs]
    earlier = iota((obs, obs), 0) < iota((obs, obs), 1)
    slot_ids = iota((ends, obs), 0)

    def stacked(kind):
        return jnp.concatenate(
            [upright[:, kind * bands + b : kind * bands + b + 1] for b in range(bands)], axis=0
        )

    marks = []
    for b in range(bands):
        row = local_int[b : b + 1]
        used = used_all[b : b + 1]
        same = (upright[:, b : b + 1] == local[b : b + 1]) & earlier
        rank = jnp.sum(jnp.where(same, 1.0, 0.0), axis=0, keepdims=True).astype(jnp.int32)
        bases = (row, row - (columns - reach), row + first - (cols_ref[b] - reach))
        mark = []
        for base in bases:
            fits = used & (base >= 0) & (base < reach)
            slot = jnp.where(fits, base * OC + rank, -1)
            mark.append(jnp.where(slot_ids == slot, 1.0, 0.0))
        marks.append(jnp.concatenate(mark, axis=0).astype(BF16))

    tapering = taper_weights(RADIUS)
    lane = iota((1, LANES), 1)
    lane_band, lane_col = lane // columns, lane % columns
    count = jnp.zeros((1, LANES), jnp.int32)
    for b in range(bands):
        count = jnp.where(lane_band == b, cols_ref[b], count)
    chooser = jnp.where(iota((LANES, LANES), 0) == lane_band, 1.0, 0.0).astype(BF16)
    source = dot(upright.astype(BF16), chooser).astype(jnp.int32)
    nth = iota((ends, LANES), 0) // OC

    def taper(place, limit):
        away = place - lane_col
        away = jnp.where(2 * away > limit, away - limit, away)
        away = jnp.where(2 * away < -limit, away + limit, away)
        away = jnp.abs(away)
        weight = jnp.zeros(place.shape, F32)
        for t in range(RADIUS):
            weight = jnp.where(away == t, tapering[t], weight)
        return weight.astype(BF16)

    near_own = taper(source, count)
    near_left = taper(nth - reach, FAR)
    near_right = taper(nth + columns, FAR)
    near_head = taper(nth + count - first, FAR)
    beside = (
        jnp.concatenate([near_right, near_head], axis=0),
        jnp.concatenate([near_left, near_head], axis=0),
    )
    weights[0] = jnp.concatenate([near_own, beside[0]], axis=0)
    weights[1] = jnp.concatenate([near_own, beside[1]], axis=0)

    spots = stacked(1).astype(jnp.int32)
    scales = stacked(2)
    depth = pairs * columns
    gathered = []
    for b in range(bands):
        index = lax.shift_right_logical(spots[b * obs : (b + 1) * obs], 1)
        onehot = jnp.where(iota((obs, depth), 1) == index, 1.0, 0.0).astype(BF16)
        x_loads[b].wait()
        field = jnp.concatenate(
            [x_v[b, :, p * LANES : (p + 1) * LANES] for p in range(pairs)], axis=0
        )
        gathered.append(dot(onehot, field))
    found = jnp.concatenate(gathered, axis=0)
    total = bands * obs
    low_t = iota((total, LANES), 1) < K
    even = (spots & 1) == 0
    picked = jnp.where(low_t == even, found, pltpu.roll(found, K, 1))
    anomaly = picked - jnp.mean(picked, axis=1, keepdims=True)
    departs = (scales * (anomaly - stacked(3))).astype(BF16)
    wide = departs.astype(F32)
    own[...] = wide
    centre = jnp.mean(wide, axis=1, keepdims=True)
    spread = wide - centre
    numerator = jnp.sum(centre * centre, axis=0, keepdims=True)
    spread_row = jnp.sum(spread * spread, axis=0, keepdims=True)
    mask_row = jnp.sum(mask, axis=0, keepdims=True)
    denominator = jnp.sum(spread_row, axis=1, keepdims=True) * (0.5 / (K - 1)) + jnp.sum(
        mask_row, axis=1, keepdims=True
    )
    stat_buf[me] = jnp.where(iota((1, LANES), 1) == 0, numerator, denominator)

    def compact_ends():
        low = iota((obs, LANES), 1) < K
        for q in range(bands // PAIR):
            mark = jnp.concatenate([marks[2 * q], marks[2 * q + 1]], axis=1)
            one = wide[(2 * q) * obs : (2 * q + 1) * obs]
            two = wide[(2 * q + 1) * obs : (2 * q + 2) * obs]
            both = jnp.concatenate(
                [jnp.where(low, one, 0.0), jnp.where(low, 0.0, two)], axis=0
            ).astype(BF16)
            compact = dot(mark, both).astype(BF16)
            for kind in range(3):
                ends_buf[kind, q] = compact[kind * ends : (kind + 1) * ends]

    soon = lon < lons // 2
    pl.when(soon)(compact_ends)

    rows_x = xs.shape[0] // columns
    groups = columns // GROUP
    low_x = iota((rows_x, LANES), 1) < K
    def spread_band(b, carry):
        for p in range(pairs):
            strip = x_v[b, :, p * LANES : (p + 1) * LANES].astype(F32)
            xs[pl.ds(p, columns, stride=rows_x), :] = strip
        for g in range(groups):
            halves = []
            for c in (g * GROUP, g * GROUP + 2):
                here = xs[c * rows_x : (c + 1) * rows_x, :]
                there = xs[(c + 1) * rows_x : (c + 2) * rows_x, :]
                halves.append(
                    jnp.concatenate(
                        [
                            jnp.where(low_x, here, pltpu.roll(there, K, 1)),
                            jnp.where(low_x, pltpu.roll(here, K, 1), there),
                        ],
                        axis=0,
                    ).astype(BF16)
                )
            x_out[b * groups + g] = jnp.concatenate(halves, axis=1)
        return carry

    eye = jnp.where(iota((K, SPAN), 0) == iota((K, SPAN), 1) % K, 1.0, 0.0)
    spare = pairs
    expand_row = iota((LANES, SPAN), 0) - iota((LANES, SPAN), 1) // K
    row_id = iota((16, SPAN), 0) + 16

    edge = -(-reach // GROUP)

    def half_gram(slot):
        spread = slot - jnp.mean(slot, axis=1, keepdims=True)
        rows = slot.shape[0]
        square = jnp.concatenate([slot, jnp.zeros((LANES - rows, LANES), F32)], axis=0)
        turned = jnp.transpose(square)[:K, :rows]
        centre = jnp.mean(turned, axis=0, keepdims=True)
        left = jnp.concatenate([turned - centre, -centre, jnp.zeros((15, rows), F32)], axis=0)
        return left.astype(BF16), spread

    def weighted(spread, wide_w):
        return jnp.concatenate(
            [
                (spread * wide_w[:, :LANES]).astype(BF16),
                (spread * wide_w[:, LANES:]).astype(BF16),
            ],
            axis=1,
        )

    def own_part(p, carry):
        made = []
        for j in range(PAIR):
            start = pl.multiple_of((p * PAIR + j) * obs, obs)
            made.append(half_gram(own[pl.ds(start, obs), :]))

        def column_group(j, g):
            i = (p * PAIR + j) * groups + g
            picker = jnp.where(
                expand_row == (p * PAIR + j) * columns + g * GROUP, 1.0, 0.0
            ).astype(BF16)
            wide_w = dot(weights[1 if g < edge else 0], picker)
            yield
            w_side[i] = wide_w[obs:]
            gram = dot(made[j][0], weighted(made[j][1], wide_w[:obs]))
            yield
            c_own[i] = gram

        wavefront([column_group(j, g) for j in range(PAIR) for g in range(groups)], GAP_OWN)
        return carry

    bands_before = jnp.where(soon, bands, 0)
    pairs_before = jnp.where(soon, bands // PAIR, 0)
    lax.fori_loop(0, bands_before, spread_band, 0)
    lax.fori_loop(0, pairs_before, own_part, 0)

    pl.semaphore_wait(barrier, devices - 1)

    def stat_copy(slot, size, other):
        return pltpu.make_async_remote_copy(
            src_ref=stat_buf.at[pl.ds(slot, size)],
            dst_ref=stat_buf.at[pl.ds(slot, size)],
            send_sem=stat_send,
            recv_sem=stat_recv,
            device_id=(other // lons, other % lons),
            device_id_type=MESH,
        )

    def near_copy(kind, slot, other):
        return pltpu.make_async_remote_copy(
            src_ref=ends_buf.at[kind],
            dst_ref=near_buf.at[slot],
            send_sem=near_send.at[slot],
            recv_sem=near_recv.at[slot],
            device_id=(lat, other),
            device_id_type=MESH,
        )

    def head_copy(other):
        return pltpu.make_async_remote_copy(
            src_ref=ends_buf.at[0],
            dst_ref=near_buf.at[2],
            send_sem=head_send.at[other],
            recv_sem=head_recv,
            device_id=(lat, other),
            device_id_type=MESH,
        )

    def tail_copy(slot):
        return pltpu.make_async_remote_copy(
            src_ref=ends_buf.at[2],
            dst_ref=tail_buf.at[slot],
            send_sem=tail_send,
            recv_sem=tail_recv,
            device_id=(lat, 0),
            device_id_type=MESH,
        )

    @pl.when(lon == 0)
    def _():
        for other in [*range(2, lons), 1]:
            head_copy(other).start()

    for other in range(devices):

        @pl.when(me != other)
        def _():
            stat_copy(me, 1, other).start()

    pl.when(jnp.logical_not(soon))(compact_ends)

    @pl.when(lon < lons - 1)
    def _():
        near_copy(1, 0, lon + 1).start()

    @pl.when(lon > 0)
    def _():
        near_copy(0, 1, lon - 1).start()
        tail_copy(lon).start()

    lax.fori_loop(bands_before, bands, spread_band, 0)
    lax.fori_loop(pairs_before, bands // PAIR, own_part, 0)

    def early(chosen, extras, block, offset):
        made = []
        low_e = iota(extras[0].shape, 1) < K
        skip = 2 * ends - extras[0].shape[0]
        for extra in extras:
            swapped = pltpu.roll(extra, K, 1)
            made.append(half_gram(jnp.where(low_e, extra, swapped)))
            made.append(half_gram(jnp.where(low_e, swapped, extra)))
        places = [(j, j * groups + g) for j in range(bands) for g in chosen]

        def column_group(line, j, i):
            gram = c_own[i] + dot(made[j][0], weighted(made[j][1], w_side[i, skip:]))
            yield
            c = gram[:K]
            c_out[i] = c
            narrow = c.astype(BF16)
            mean = gram[K : K + 1]
            old = x_out[i]
            middle = jnp.where(row_id == spare, mean, old[16:32].astype(F32)).astype(BF16)
            field = jnp.concatenate([old[:16], middle, old[32:]], axis=0)
            x_out[i] = field
            norm[block, 0, line : line + 1, :] = jnp.sum(c * c, axis=0, keepdims=True)
            norm[block, 1, line : line + 1, :] = jnp.sum(c * eye, axis=0, keepdims=True)
            both = dot(jnp.concatenate([narrow, field], axis=0), block_diag(narrow))
            yield
            s_out[i] = both[:K]
            p_out[i] = both[K:]
            cube = dot(narrow, block_diag(both[:K].astype(BF16)))
            yield
            q_out[i] = cube

        return [column_group(offset + n, j, i) for n, (j, i) in enumerate(places)]

    @pl.when(lon > 0)
    def _():
        head_copy(lon).wait_recv()

    halves = bands // PAIR
    centre_groups = range(edge, groups - edge)
    heads = [near_buf[2, p].astype(F32) for p in range(halves)]
    wavefront(early(centre_groups, heads, 0, 0), GAP_EARLY)

    @pl.when(lon < lons - 1)
    def _():
        near_copy(0, 1, lon + 1).wait_recv()

    rights = [
        jnp.concatenate([near_buf[1, p].astype(F32), heads[p]], axis=0) for p in range(halves)
    ]
    left_groups, right_groups = range(edge), range(groups - edge, groups)
    wavefront(early(right_groups, rights, 1, 0), GAP_EARLY)

    def settle(block, shift, sums):
        inv = lax.rsqrt(sums[0] + shift * (2.0 * sums[1] + K * shift))
        scaling = jnp.sqrt((K - 1.0) * inv)
        beta = 1.0 - shift * inv
        beta1 = beta * beta * (0.75 + 0.25 * beta)
        beta2 = beta1 * beta1 * (0.75 + 0.25 * beta1)
        a0 = 1.0 + 0.5 * beta
        a1 = 1.0 + 0.5 * beta1
        half1 = 0.5 / a1
        c0 = (1.0 + 0.5 * beta2) * (1.0 + (0.375 + 0.125 * beta2) * beta2 * beta2)
        c1 = 0.5 + beta2 * (0.75 + beta2 * (0.9375 + 0.25 * beta2))
        c2 = 0.375 + beta2 * (0.9375 + 0.375 * beta2)
        c3 = 0.3125 + 0.25 * beta2
        up, down = c1 / c0, c0 / c1
        whole = a0 * a1 * c0
        table = (
            -inv * (1.5 * beta + 0.75 * beta * beta) * half1,
            inv * inv * (0.75 + 0.75 * beta) * half1,
            -0.25 * inv * inv * inv * half1,
            -0.5 * inv / a0,
            2.0 * a1 * up * (1.5 * beta1 + 0.75 * beta1 * beta1),
            4.0 * a1 * a1 * up * (0.75 + 0.75 * beta1),
            2.0 * a1 * a1 * a1 * up,
            c2 / c0 * down * down,
            c3 / c0 * down * down * down,
            0.0625 / c0 * (down * down) * (down * down),
            whole * whole * inv,
            (1.0 - scaling * whole) * (1.0 / K),
            scaling * whole,
        )
        for t, value in enumerate(table):
            coef[block, t] = value

    def finish(work):
        def k(t, w):
            return coef[w[0], t, w[1] : w[1] + 1, :]

        def wide_x(w):
            return x_out[w[2]].astype(F32)

        held = {}

        def column_group(n, w):
            i = w[2]
            m = k(0, w) * c_out[i] + k(1, w) * s_out[i] + k(2, w) * q_out[i]
            x = wide_x(w) + k(3, w) * p_out[i]
            m_b = m.astype(BF16)
            both = dot(jnp.concatenate([m_b, x.astype(BF16)], axis=0), block_diag(m_b))
            yield
            square = both[:K]
            cube = dot(m_b, block_diag(square.astype(BF16)))
            x = x + both[K:]
            yield
            m_b = (k(4, w) * m + k(5, w) * square + k(6, w) * cube).astype(BF16)
            x_b = x.astype(BF16)
            both = dot(jnp.concatenate([m_b, x_b], axis=0), block_diag(m_b))
            yield
            fixed = block_diag(both[:K].astype(BF16))
            quad = dot(x_b, fixed)
            part = k(7, w) * x + k(8, w) * both[K:]
            x = x + both[K:]
            yield
            last = dot((part + k(9, w) * quad).astype(BF16), fixed)
            yield
            x = x + last
            step = x[spare : spare + 1] * k(10, w)
            held[n] = (x * step + wide_x(w) * k(11, w)).astype(BF16)
            if n % SHARED == SHARED - 1 or n + 1 == len(work):
                first_n = n - n % SHARED
                stack = jnp.concatenate([held[v] for v in range(first_n, n + 1)], axis=0)
                means = dot(stack, ones_bd)
                rows = stack.shape[0] // (n + 1 - first_n)
                for v in range(first_n, n + 1):
                    held[v] = means[(v - first_n) * rows : (v - first_n + 1) * rows]
            yield
            yield
            result = k(12, w) * x + held[n]
            b, g = i // groups, i % groups
            for side in range(2):
                c = g * GROUP + 2 * side
                got = result[:, side * LANES : (side + 1) * LANES]
                evens, odds = got[:rows_x], got[rows_x:]
                r_out[b, c * rows_x : (c + 1) * rows_x, :] = jnp.where(
                    low_x, evens, pltpu.roll(odds, K, 1)
                )
                r_out[b, (c + 1) * rows_x : (c + 2) * rows_x, :] = jnp.where(
                    low_x, pltpu.roll(evens, K, 1), odds
                )

        return [column_group(n, w) for n, w in enumerate(work)]

    def lines(block, offset, chosen):
        places = [b * groups + g for b in range(bands) for g in chosen]
        return [(block, offset + n, i) for n, i in enumerate(places)]

    ones_bd = block_diag(jnp.ones((K, SPAN), BF16))

    def block_sums(block):
        both = jnp.concatenate([norm[block, 0], norm[block, 1]], axis=0)
        coarse = both.astype(BF16)
        fine = (both - coarse.astype(F32)).astype(BF16)
        size = both.shape[0]
        sums = dot(jnp.concatenate([coarse, fine], axis=0), ones_bd)
        sums = sums[:size] + sums[size:]
        return sums[: size // 2], sums[size // 2 :]

    first_sums = block_sums(0)
    everyone = stat_copy(0, devices - 1, 0)
    everyone.wait_send()
    everyone.wait_recv()
    stats = jnp.sum(stat_buf[...], axis=0)
    inflation = (stats[:, 0:1] + 1e-06) / stats[:, 1:2]
    shift = (K - 1) / inflation
    line = iota((8, LANES), 0)
    info = jnp.zeros((8, LANES), F32)
    for b in range(bands):
        info = jnp.where(line == b, (cols_ref[b] - first).astype(F32), info)
    info_out[...] = info
    settle(0, shift, first_sums)
    wavefront(finish(lines(0, 0, centre_groups)), GAP_LATE)

    @pl.when(lon > 0)
    def _():
        near_copy(1, 0, lon - 1).wait_recv()

    @pl.when(lon == 0)
    def _():
        pltpu.make_async_remote_copy(
            src_ref=tail_buf.at[pl.ds(1, lons - 1)],
            dst_ref=tail_buf.at[pl.ds(1, lons - 1)],
            send_sem=tail_send,
            recv_sem=tail_recv,
            device_id=(lat, 0),
            device_id_type=MESH,
        ).wait_recv()

    lefts = []
    for p in range(halves):
        ahead = near_buf[0, p].astype(F32)
        for other in range(1, lons):
            ahead = ahead + tail_buf[other, p].astype(F32)
        lefts.append(jnp.concatenate([ahead, heads[p]], axis=0))
    wavefront(early(left_groups, lefts, 1, bands * edge), GAP_EARLY)
    settle(1, shift, block_sums(1))
    wavefront(
        finish(lines(1, 0, right_groups) + lines(1, bands * edge, left_groups)), GAP_LATE
    )

    @pl.when(lon > 0)
    def _():
        tail_copy(lon).wait_send()
        near_copy(0, 1, lon - 1).wait_send()

    @pl.when(lon == 0)
    def _():
        for other in range(1, lons):
            head_copy(other).wait_send()

    @pl.when(lon < lons - 1)
    def _():
        near_copy(1, 0, lon + 1).wait_send()


def layout_kernel(r_ref, info_ref, out_hbm, obuf, out_sem):
    bands, columns, width = obuf.shape
    pairs = width // LANES
    rows_x = r_ref.shape[1] // columns

    def write(b):
        return pltpu.make_async_copy(obuf.at[b], out_hbm.at[b], out_sem.at[b])

    for b in range(bands):
        keep = iota((columns, LANES), 0).astype(F32) < info_ref[b : b + 1, :]
        for t in range(pairs):
            obuf[b, :, t * LANES : (t + 1) * LANES] = jnp.where(
                keep, r_ref[b, pl.ds(t, columns, stride=rows_x), :], 0.0
            ).astype(BF16)
        write(b).start()
    for b in range(bands):
        write(b).wait()


def per_device(lats, lons, background, band_cols, obs_col, obs_lev, obs_mask, innov, obs_var):
    bands, columns, width = background.shape
    obs = obs_col.shape[1]
    pairs = width // LANES
    devices = lats * lons
    vmem = pl.BlockSpec(memory_space=pltpu.VMEM)
    hbm = pl.BlockSpec(memory_space=pltpu.HBM)
    dma = pltpu.SemaphoreType.DMA
    rows_x = -(-(pairs + 1) // 8) * 8
    halves = bands // PAIR
    slots = obs + 2 * END_SLOTS
    total = bands * columns // GROUP
    rim = 2 * -(-(RADIUS - 1) // GROUP) * bands
    most = -(-max(rim, total - rim) // 8) * 8
    room = 16 * 1024 * 1024
    arrays = (background, obs_col, obs_lev, obs_mask, innov, obs_var, band_cols)
    groups_f32 = pltpu.VMEM((total, K, SPAN), F32)
    result, info = pl.pallas_call(
        functools.partial(exchange_kernel, lats, lons),
        out_shape=(
            jax.ShapeDtypeStruct((bands, columns * rows_x, LANES), F32),
            jax.ShapeDtypeStruct((8, LANES), F32),
        ),
        in_specs=[hbm] * 7,
        out_specs=(vmem,) * 2,
        scratch_shapes=[
            groups_f32,
            groups_f32,
            groups_f32,
            pltpu.VMEM((total, 2 * rows_x, SPAN), F32),
            pltpu.VMEM((total, 2 * rows_x, SPAN), BF16),
            pltpu.VMEM((2, 2, most, SPAN), F32),
            pltpu.VMEM((2, 13, most, SPAN), F32),
            pltpu.VMEM((bands, columns, width), BF16),
            pltpu.VMEM((bands, obs), jnp.int32),
            pltpu.VMEM((bands, obs), jnp.int32),
            pltpu.VMEM((bands, obs), jnp.int32),
            pltpu.VMEM((bands, obs), F32),
            pltpu.VMEM((bands, obs), F32),
            pltpu.SMEM((bands,), jnp.int32),
            pltpu.VMEM((columns * rows_x, LANES), F32),
            pltpu.VMEM((bands * obs, LANES), F32),
            pltpu.VMEM((2, slots, LANES), BF16),
            pltpu.VMEM((total, 2 * END_SLOTS, SPAN), F32),
            pltpu.VMEM((total, K + 16, SPAN), F32),
            pltpu.VMEM((3, halves, END_SLOTS, LANES), BF16),
            pltpu.VMEM((3, halves, END_SLOTS, LANES), BF16),
            pltpu.VMEM((lons, halves, END_SLOTS, LANES), BF16),
            pltpu.VMEM((devices, 1, LANES), F32),
            dma((bands,)),
            dma((6,)),
            dma((2,)),
            dma((2,)),
            dma((lons,)),
            dma,
            dma,
            dma,
            dma,
            dma,
        ],
        compiler_params=pltpu.CompilerParams(
            collective_id=0, has_side_effects=True, vmem_limit_bytes=2 * room
        ),
        name="exchange",
    )(*(pltpu.with_memory_space_constraint(a, pltpu.HBM) for a in arrays))
    return pl.pallas_call(
        layout_kernel,
        out_shape=jax.ShapeDtypeStruct(background.shape, BF16),
        in_specs=[vmem] * 2,
        out_specs=hbm,
        scratch_shapes=[
            pltpu.VMEM((bands, columns, width), BF16),
            dma((bands,)),
        ],
        compiler_params=pltpu.CompilerParams(vmem_limit_bytes=room),
        name="layout",
    )(result, info)


def solution(mesh):
    placed = (P("lat", "lon", None), P("lat")) + (P("lat", "lon"),) * 5
    return jax.shard_map(
        functools.partial(per_device, mesh.shape["lat"], mesh.shape["lon"]),
        mesh=mesh,
        in_specs=placed,
        out_specs=P("lat", "lon", None),
        check_vma=False,
    )
```
